32 devices in a mesh: dp: 4 (over x, core), mp: 8 (over z, y).
Axes of the slice: x: 2, y: 2, z: 4, core: 2. Of those that a mesh axis runs over, the one named last changes fastest.
Arguments:
- tokens: bfloat16 [3072, 6144], P('dp'), may hold values from -60 to 60
- ln_gain: float32 [6144], replicated, may hold values from 0.1 to 1.9
- w_qkv: bfloat16 [6144, 3, 6144], P('dp', None, 'mp'), may hold values from -1 to 1
- q_gain: float32 [128], replicated, may hold values from 0.7 to 2
- k_gain: float32 [128], replicated, may hold values from 0.7 to 2
Outputs:
- context: bfloat16 [3072, 6144], P('dp', 'mp')
The draws below stay inside these ranges and needn't reach their ends.
All inputs are finite; a program needn't handle non-finite values.
Results may differ from the reference program's by a relative error of at most 0.012.
The reference program's roundings to bfloat16 on the way count: a program that leaves them out, or rounds other values in their place, can miss the bound.
Values may be sent and summed in bfloat16 or wider, within the bound.
A program may use at most 128 MiB of HBM per device.

```python
import jax
import jax.numpy as jnp
from jax import lax

D = 6144
HEADS = 48
HEAD_DIM = 128
PATCHES = 256
SPLITS = 4
IMAGES = 12
TOKENS = 3072


def draw_tokens(key, part):
    subkeys = jax.random.split(key, 3)
    row_scale = jnp.exp(jax.random.uniform(subkeys[0], (TOKENS, 1), jnp.float32, -1.2, 1.2))
    col_scale = jnp.exp(jax.random.uniform(subkeys[1], (1, D), jnp.float32, -1.2, 1.2))
    base_draw = jnp.clip(jax.random.normal(subkeys[2], (TOKENS, D), jnp.float32), -4.0, 4.0)
    values = base_draw * row_scale * col_scale
    return jnp.clip(values, -60.0, 60.0).astype(jnp.bfloat16)


def draw_w_qkv(key, part):
    subkeys = jax.random.split(key, 2)
    col_scale = jnp.exp(jax.random.uniform(subkeys[0], (1, 3, D), jnp.float32, -1.0, 1.2))
    base_draw = jnp.clip(jax.random.normal(subkeys[1], (D, 3, D), jnp.float32), -4.0, 4.0)
    values = base_draw * col_scale * D ** (-0.5)
    return jnp.clip(values, -1.0, 1.0).astype(jnp.bfloat16)


def setup_inputs(seed: int = 0) -> dict:
    key_of = jax.random.split(jax.random.key(seed), 6)
    tokens = draw_tokens(jax.random.fold_in(key_of[5], 71), 0)
    ln_gain = jnp.clip(1.0 + 0.18 * jax.random.normal(key_of[1], (D,), jnp.float32), 0.1, 1.9)
    w_qkv = draw_w_qkv(jax.random.fold_in(key_of[5], 71), 0)
    q_gain = jnp.clip(jax.random.uniform(key_of[3], (HEAD_DIM,), jnp.float32, 0.7, 2.0), 0.7, 2.0)
    k_gain = jnp.clip(jax.random.uniform(key_of[4], (HEAD_DIM,), jnp.float32, 0.7, 2.0), 0.7, 2.0)
    return {"tokens": tokens, "ln_gain": ln_gain, "w_qkv": w_qkv, "q_gain": q_gain, "k_gain": k_gain}


norm_eps = 1e-06

def layer_norm(values, gain_vector):
    centre = lax.optimization_barrier(jnp.mean(values, axis=-1, keepdims=True))
    centred = values - centre
    spread = lax.optimization_barrier(jnp.mean(centred * centred, axis=-1, keepdims=True))
    return centred * lax.rsqrt(spread + norm_eps) * gain_vector

def to_heads(features):
    leading = features.shape[:-1]
    parted = features.reshape(leading + (SPLITS, HEADS, HEAD_DIM // SPLITS))
    swapped = jnp.moveaxis(parted, -3, -2)
    return swapped.reshape(leading + (HEADS, HEAD_DIM))

def from_heads(features):
    leading = features.shape[:-2]
    parted = features.reshape(leading + (HEADS, SPLITS, HEAD_DIM // SPLITS))
    swapped = jnp.moveaxis(parted, -2, -3)
    return swapped.reshape(leading + (D,))

def reference(tokens, ln_gain, w_qkv, q_gain, k_gain):
    normed = layer_norm(tokens.astype(jnp.float32), ln_gain).astype(jnp.bfloat16)
    projected = jnp.dot(normed, w_qkv.reshape(D, 3 * D), preferred_element_type=jnp.float32).astype(jnp.bfloat16)
    projected = projected.reshape(IMAGES, PATCHES, 3, D)

    def attend(one_image):
        per_head = to_heads(one_image)
        queries = (layer_norm(per_head[:, 0].astype(jnp.float32), q_gain) * HEAD_DIM ** (-0.5)).astype(jnp.bfloat16)
        key_vecs = layer_norm(per_head[:, 1].astype(jnp.float32), k_gain).astype(jnp.bfloat16)
        values = per_head[:, 2]
        scores = jnp.einsum('qhe,khe->hqk', queries.astype(jnp.float32), key_vecs.astype(jnp.float32))
        raised = jnp.exp(scores)
        weights = (raised / lax.optimization_barrier(jnp.sum(raised, axis=-1, keepdims=True))).astype(jnp.bfloat16)
        attended = jnp.einsum('hqk,khe->qhe', weights.astype(jnp.float32), values.astype(jnp.float32)).astype(jnp.bfloat16)
        return from_heads(attended)
    context = lax.map(attend, projected)
    return context.reshape(TOKENS, D)
```

```python
import functools

import jax
import jax.numpy as jnp
from jax import lax
from jax.experimental import pallas as pl
from jax.experimental.pallas import tpu as pltpu
from jax.sharding import PartitionSpec as P


HEADS = 48
HEAD_DIM = 128
PATCHES = 256
SPLITS = 4


norm_eps = 1e-06


def from_behind(shard, axis, by):
    length = lax.axis_size(axis)
    return lax.ppermute(shard, axis, [(i, (i + by) % length) for i in range(length)])


def layer_norm(values, gain_vector):
    centre = jnp.mean(values, axis=-1, keepdims=True)
    centred = values - centre
    spread = jnp.mean(centred * centred, axis=-1, keepdims=True)
    return centred * lax.rsqrt(spread + norm_eps) * gain_vector


def head_norm(pieces, gain_rows):
    values = pieces.astype(jnp.float32)
    centre = jnp.mean(values, axis=(0, 4), keepdims=True)
    centred = values - centre
    spread = jnp.mean(centred * centred, axis=(0, 4), keepdims=True)
    return centred * lax.rsqrt(spread + norm_eps) * gain_rows[:, None, None, None, :]


def ordered_gains(gain_vector, quarter_order):
    gain_table = gain_vector.reshape(SPLITS, -1)
    selector = (quarter_order[:, None] == jnp.arange(SPLITS, dtype=jnp.int32)[None, :]).astype(
        jnp.float32
    )
    return jnp.dot(selector, gain_table, precision=lax.Precision.HIGHEST)


def plain_body(tokens, ln_gain, w_qkv, q_gain, k_gain):
    local_rows = tokens.shape[0]
    normed = layer_norm(tokens.astype(jnp.float32), ln_gain).astype(jnp.bfloat16)
    flat_weight = w_qkv.reshape(w_qkv.shape[0], -1)
    out_width = flat_weight.shape[1]
    row_piece = lax.all_gather(w_qkv, "dp", axis=0, tiled=True)
    partial_value = jnp.dot(
        normed, row_piece.reshape(row_piece.shape[0], out_width), preferred_element_type=jnp.float32
    )
    projected = partial_value.astype(jnp.bfloat16)
    groups = lax.axis_size("mp") // SPLITS
    head_count = HEADS // groups
    quarter_rows = PATCHES // SPLITS
    my_quarter = lax.axis_index("mp") // groups
    images = local_rows // PATCHES
    head_view = projected.reshape(images, PATCHES, 3, head_count, HEAD_DIM // SPLITS)
    queries = head_view[:, :, 0]
    keys_vals = head_view[:, :, 1:]
    counting = jnp.arange(SPLITS, dtype=jnp.int32)
    own_rows = lax.dynamic_slice_in_dim(queries, my_quarter * quarter_rows, quarter_rows, 1)
    query_list = [own_rows]
    pair_list = [keys_vals]
    for offset in range(1, SPLITS):
        outgoing = lax.dynamic_slice_in_dim(
            queries, (my_quarter + offset) % SPLITS * quarter_rows, quarter_rows, 1
        )
        got_query, got_pair = from_behind((outgoing, keys_vals), "mp", offset * groups)
        query_list.append(got_query)
        pair_list.append(got_pair)
    query_pieces = jnp.stack(query_list, 0)
    pair_pieces = jnp.stack(pair_list, 0)
    quarter_order = (my_quarter - counting) % SPLITS
    query_normed = (
        head_norm(query_pieces, ordered_gains(q_gain, quarter_order)) * HEAD_DIM ** (-0.5)
    ).astype(jnp.bfloat16)
    key_normed = head_norm(pair_pieces[:, :, :, 0], ordered_gains(k_gain, quarter_order)).astype(
        jnp.bfloat16
    )
    value_part = pair_pieces[:, :, :, 1]
    scores = jnp.einsum(
        "sirhe,sikhe->ihrk", query_normed, key_normed, preferred_element_type=jnp.float32
    )
    raised = jnp.exp(scores)
    weights = (raised / jnp.sum(raised, axis=-1, keepdims=True)).astype(jnp.bfloat16)
    context = jnp.einsum(
        "ihrk,sikhe->sirhe", weights, value_part, preferred_element_type=jnp.float32
    ).astype(jnp.bfloat16)
    rows_list = [context[0]]
    for offset in range(1, SPLITS):
        wanted = (my_quarter - offset) % SPLITS
        slot_index = jnp.sum(jnp.where(quarter_order == wanted, counting, 0))
        outgoing = lax.dynamic_index_in_dim(context, slot_index, 0, keepdims=False)
        rows_list.append(from_behind(outgoing, "mp", (SPLITS - offset) * groups))
    own_block = jnp.roll(jnp.concatenate(rows_list, 1), my_quarter * quarter_rows, axis=1)
    return own_block.reshape(local_rows, -1)

MESH = pl.DeviceIdType.MESH
VMEM_LIMIT = 62 * 1024 * 1024
KINDS = 3
BLOCK = 256
SHARERS = 4
LAG_SUM, LAG_ATTEND, LAG_STORE = 1, 3, 5


def column_norm(values, gain_column):
    centre = jnp.mean(values, axis=0, keepdims=True)
    centred = values - centre
    spread = jnp.mean(centred * centred, axis=0, keepdims=True)
    return centred * lax.rsqrt(spread + norm_eps) * gain_column


def span(start, size):
    return pl.ds(pl.multiple_of(start, size), size)


def fused_kernel(
    token_hbm, gain_ref, weight_hbm, q_gain_ref, k_gain_ref, out_ref,
    work, weight, own, other, share, total, partial, pieces, returned,
    token_in, weight_in, weight_out, weight_got, share_out, share_got,
    relay_out, relay_got, partial_out, partial_got, piece_out, piece_got,
    context_out, context_got,
):
    dp, mp = lax.axis_index("dp"), lax.axis_index("mp")
    groups = lax.axis_size("mp") // SPLITS
    side, core = dp // 2, dp % 2
    quarter, group = mp // groups, mp % groups
    rows, features = token_hbm.shape
    width = weight_hbm.shape[2]
    depth = weight_hbm.shape[1]
    half = features // 2
    images, blocks = rows // PATCHES, width // BLOCK
    chunks = images * blocks
    part = HEAD_DIM // SPLITS
    height = BLOCK // SPLITS
    heads = height // part
    share_rows = PATCHES // SHARERS

    sibling = (side * 2 + 1 - core, mp)
    across = ((1 - side) * 2 + core, mp)
    near_group = (dp, quarter * groups + 1 - group)
    pair = quarter + 1 - 2 * (quarter % 2)
    near_quarter = (dp, pair * groups + group)
    diagonal = (dp, pair * groups + 1 - group)
    relays = (near_group, near_quarter, diagonal)

    def quarter_at(offset):
        return (dp, (quarter + offset) % SPLITS * groups + group)

    def remote(source, target, send, receive, device):
        return pltpu.make_async_remote_copy(
            src_ref=source, dst_ref=target, send_sem=send, recv_sem=receive,
            device_id=device, device_id_type=MESH,
        )

    def token_load(image):
        lines = span(image * PATCHES, PATCHES)
        return pltpu.make_async_copy(token_hbm.at[lines], work.at[lines], token_in.at[image])

    mine = span(core * depth, depth)

    def weight_load(block):
        columns = span(block * BLOCK, BLOCK)
        return pltpu.make_async_copy(
            weight_hbm.at[:, :, columns], weight.at[:, mine, columns], weight_in.at[block]
        )

    def weight_send(block):
        columns = span(block * BLOCK, BLOCK)
        return remote(
            weight_hbm.at[:, :, columns], weight.at[:, mine, columns],
            weight_out.at[block], weight_got.at[block], sibling,
        )

    place = quarter % 2 * 2 + group

    def share_send(image):
        return remote(
            share.at[image], other.at[span(image * PATCHES + place * share_rows, share_rows)],
            share_out.at[image], share_got.at[image], across,
        )

    def relay_send(image, way):
        lines = span(image * PATCHES + place * share_rows, share_rows)
        return remote(
            other.at[lines], other.at[lines],
            relay_out.at[image * 3 + way], relay_got.at[image * 3 + way], relays[way],
        )

    def partial_send(chunk):
        image, block = chunk // blocks, chunk % blocks
        return remote(
            work.at[span(image * PATCHES, PATCHES), span(block * KINDS * BLOCK, KINDS * BLOCK)],
            partial.at[chunk], partial_out.at[chunk], partial_got.at[chunk], across,
        )

    def piece_source(chunk, destination):
        image, block = chunk // blocks, chunk % blocks
        first = KINDS * width
        return work.at[
            span(image * PATCHES + destination * height, height),
            span(first + block * KINDS * BLOCK, KINDS * BLOCK),
        ]

    def piece_send(chunk, offset):
        slot = chunk * 3 + offset - 1
        return remote(
            piece_source(chunk, (quarter + offset) % SPLITS), pieces.at[chunk, quarter],
            piece_out.at[slot], piece_got.at[slot], quarter_at(offset),
        )

    def context_source(chunk, destination):
        image, block = chunk // blocks, chunk % blocks
        first = 2 * KINDS * width
        return work.at[
            span(image * PATCHES + destination * height, height),
            span(first + block * BLOCK, BLOCK),
        ]

    def context_send(chunk, offset):
        slot = chunk * 3 + offset - 1
        return remote(
            context_source(chunk, (quarter + offset) % SPLITS), returned.at[chunk, quarter],
            context_out.at[slot], context_got.at[slot], quarter_at(offset),
        )

    for image in range(images):
        token_load(image).start()
    for block in range(blocks):
        weight_load(block).start()
    barrier = pltpu.get_barrier_semaphore()
    partners = [sibling, across, near_group, diagonal] + [quarter_at(o) for o in range(1, SPLITS)]
    for partner in partners:
        pl.semaphore_signal(barrier, inc=1, device_id=partner, device_id_type=MESH)
    pl.semaphore_wait(barrier, len(partners))
    for block in range(blocks):
        weight_send(block).start()

    own_half = span(side * half, half)
    other_half = span((1 - side) * half, half)

    def normalize(image, turn, sharing):
        lines = span(image * PATCHES + (place + turn) % SHARERS * share_rows, share_rows)
        values = work[lines, :].astype(jnp.float32)
        centre = jnp.mean(values, axis=-1, keepdims=True)
        centred = values - centre
        spread = jnp.mean(centred * centred, axis=-1, keepdims=True)
        scale = lax.rsqrt(spread + norm_eps)

        def scaled(columns):
            return (
                (work[lines, columns].astype(jnp.float32) - centre) * scale * gain_ref[:, columns]
            ).astype(jnp.bfloat16)

        if sharing:
            share[image] = scaled(other_half)
        own[lines, :] = scaled(own_half)

    def first_norm(image, carry):
        token_load(image).wait()
        normalize(image, 0, True)
        share_send(image).start()
        return carry

    lax.fori_loop(0, images, first_norm, 0)

    def later_norm(step, carry):
        normalize(step // (SHARERS - 1), step % (SHARERS - 1) + 1, False)
        return carry

    lax.fori_loop(0, images * (SHARERS - 1), later_norm, 0)

    def relay(image):
        share_send(image).wait_recv()
        for way in range(3):
            relay_send(image, way).start()

    def own_part(step, carry):
        block, kind = step // KINDS, step % KINDS

        @pl.when(kind == 0)
        def _():
            weight_load(block).wait()
            weight_send(block).wait_recv()

        total[:, span(step * BLOCK, BLOCK)] = jnp.dot(
            own[...], weight[kind, :, span(block * BLOCK, BLOCK)],
            preferred_element_type=jnp.float32,
        )

        @pl.when(kind == KINDS - 1)
        def _():
            relay(block)

        return carry

    lax.fori_loop(0, blocks * KINDS, own_part, 0)

    def send_partial(chunk):
        image, block = chunk // blocks, chunk % blocks

        @pl.when(block == 0)
        def _():
            for way in range(3):
                relay_send(image, way).wait_recv()

        lines = span(image * PATCHES, PATCHES)
        for kind in range(KINDS):
            term = jnp.dot(
                other[lines, :], weight[kind, :, span(block * BLOCK, BLOCK)],
                preferred_element_type=jnp.float32,
            )
            work[lines, span((block * KINDS + kind) * BLOCK, BLOCK)] = term.astype(jnp.bfloat16)
        partial_send(chunk).start()

    def sum_up(chunk):
        image, block = chunk // blocks, chunk % blocks
        partial_send(chunk).wait_recv()
        lines = span(image * PATCHES, PATCHES)
        first = KINDS * width
        for kind in range(KINDS):
            columns = (block * KINDS + kind) * BLOCK
            whole = total[lines, span(columns, BLOCK)] + partial[
                chunk, :, kind * BLOCK : (kind + 1) * BLOCK
            ].astype(jnp.float32)
            work[lines, span(first + columns, BLOCK)] = whole.T.astype(jnp.bfloat16)
        for offset in range(1, SPLITS):
            piece_send(chunk, offset).start()
        pieces[chunk, quarter] = piece_source(chunk, quarter)[...]

    def attend(chunk):
        image, block = chunk // blocks, chunk % blocks
        for offset in range(1, SPLITS):
            source = (quarter - offset + SPLITS) % SPLITS
            slot = chunk * 3 + offset - 1
            remote(
                pieces.at[chunk, source], pieces.at[chunk, source],
                piece_out.at[slot], piece_got.at[slot], quarter_at(offset),
            ).wait_recv()
        for head in range(heads):
            def gathered(kind):
                return jnp.concatenate(
                    [
                        pieces[
                            chunk, source, head * part : (head + 1) * part,
                            kind * BLOCK : (kind + 1) * BLOCK,
                        ]
                        for source in range(SPLITS)
                    ],
                    axis=0,
                )

            query = (
                column_norm(gathered(0).astype(jnp.float32), q_gain_ref[...]) * HEAD_DIM ** (-0.5)
            ).astype(jnp.bfloat16)
            key = column_norm(gathered(1).astype(jnp.float32), k_gain_ref[...]).astype(jnp.bfloat16)
            scores = lax.dot_general(
                key, query, (((0,), (0,)), ((), ())), preferred_element_type=jnp.float32
            )
            raised = jnp.exp(scores)
            weights = (raised / jnp.sum(raised, axis=0, keepdims=True)).astype(jnp.bfloat16)
            attended = jnp.dot(gathered(2), weights, preferred_element_type=jnp.float32).astype(
                jnp.bfloat16
            )
            columns = span(2 * KINDS * width + block * BLOCK, BLOCK)
            for target in range(SPLITS):
                line = image * PATCHES + target * height + head * part
                work[span(line, part), columns] = attended[target * part : (target + 1) * part]
        for offset in range(1, SPLITS):
            context_send(chunk, offset).start()
        returned[chunk, quarter] = context_source(chunk, quarter)[...]

    def store(chunk):
        image, block = chunk // blocks, chunk % blocks
        for offset in range(1, SPLITS):
            source = (quarter - offset + SPLITS) % SPLITS
            slot = chunk * 3 + offset - 1
            remote(
                returned.at[chunk, source], returned.at[chunk, source],
                context_out.at[slot], context_got.at[slot], quarter_at(offset),
            ).wait_recv()
        upright = returned[chunk].reshape(BLOCK, PATCHES)
        out_ref[span(image * PATCHES, PATCHES), span(block * BLOCK, BLOCK)] = upright.T

    def step(turn, carry):
        for lag, stage in (
            (0, send_partial), (LAG_SUM, sum_up), (LAG_ATTEND, attend), (LAG_STORE, store)
        ):
            @pl.when((turn >= lag) & (turn < chunks + lag))
            def _(lag=lag, stage=stage):
                stage(turn - lag)

        return carry

    lax.fori_loop(0, chunks + LAG_STORE, step, 0)

    for block in range(blocks):
        weight_send(block).wait_send()

    def drain(image, carry):
        share_send(image).wait_send()
        for way in range(3):
            relay_send(image, way).wait_send()
        return carry

    lax.fori_loop(0, images, drain, 0)

    def drain_chunk(chunk, carry):
        partial_send(chunk).wait_send()
        for offset in range(1, SPLITS):
            piece_send(chunk, offset).wait_send()
            context_send(chunk, offset).wait_send()
        return carry

    lax.fori_loop(0, chunks, drain_chunk, 0)


def fused(tokens, gain, weights, q_gain, k_gain):
    rows, features = tokens.shape
    kinds, depth, width = weights.shape
    images, blocks = rows // PATCHES, width // BLOCK
    chunks = images * blocks
    height = BLOCK // SPLITS
    whole = pl.BlockSpec(memory_space=pltpu.VMEM)
    outside = pl.BlockSpec(memory_space=pl.ANY)
    dma = pltpu.SemaphoreType.DMA

    def vmem(*shape, dtype=jnp.bfloat16):
        return pltpu.VMEM(shape, dtype)

    return pl.pallas_call(
        fused_kernel,
        out_shape=jax.ShapeDtypeStruct((rows, width), jnp.bfloat16),
        in_specs=[outside, whole, outside, whole, whole],
        out_specs=whole,
        scratch_shapes=[
            vmem(rows, features),
            vmem(kinds, 2 * depth, width),
            vmem(rows, features // 2),
            vmem(rows, features // 2),
            vmem(images, PATCHES // SHARERS, features // 2),
            vmem(rows, kinds * width, dtype=jnp.float32),
            vmem(chunks, PATCHES, kinds * BLOCK),
            vmem(chunks, SPLITS, height, kinds * PATCHES),
            vmem(chunks, SPLITS, height, PATCHES),
            dma((images,)), dma((blocks,)),
            dma((blocks,)), dma((blocks,)),
            dma((images,)), dma((images,)),
            dma((images * 3,)), dma((images * 3,)),
            dma((chunks,)), dma((chunks,)),
            dma((chunks * 3,)), dma((chunks * 3,)),
            dma((chunks * 3,)), dma((chunks * 3,)),
        ],
        compiler_params=pltpu.CompilerParams(
            collective_id=0, has_side_effects=True, vmem_limit_bytes=VMEM_LIMIT
        ),
        name="fused",
    )(tokens, gain.reshape(1, features), weights, q_gain.reshape(HEAD_DIM, 1),
      k_gain.reshape(HEAD_DIM, 1))


def body(tokens, ln_gain, w_qkv, q_gain, k_gain):
    return fused(tokens, ln_gain, jnp.transpose(w_qkv, (1, 0, 2)), q_gain, k_gain)


def solution(mesh):
    local_heads = HEADS * SPLITS // mesh.shape["mp"]
    columns = local_heads * (HEAD_DIM // SPLITS)
    fits = columns % BLOCK == 0 and mesh.shape["mp"] == 2 * SPLITS
    fits = fits and mesh.shape["dp"] == 4
    return jax.shard_map(
        body if fits else plain_body,
        mesh=mesh,
        in_specs=(P("dp", None), P(), P("dp", None, "mp"), P(), P()),
        out_specs=P("dp", "mp"),
        check_vma=False,
    )
```

```python
import functools

import jax
import jax.numpy as jnp
from jax import lax
from jax.experimental import pallas as pl
from jax.experimental.pallas import tpu as pltpu
from jax.sharding import PartitionSpec as P


HEADS = 48
HEAD_DIM = 128
PATCHES = 256
SPLITS = 4


norm_eps = 1e-06


def from_behind(shard, axis, by):
    length = lax.axis_size(axis)
    return lax.ppermute(shard, axis, [(i, (i + by) % length) for i in range(length)])


def layer_norm(values, gain_vector):
    centre = jnp.mean(values, axis=-1, keepdims=True)
    centred = values - centre
    spread = jnp.mean(centred * centred, axis=-1, keepdims=True)
    return centred * lax.rsqrt(spread + norm_eps) * gain_vector


def head_norm(pieces, gain_rows):
    values = pieces.astype(jnp.float32)
    centre = jnp.mean(values, axis=(0, 4), keepdims=True)
    centred = values - centre
    spread = jnp.mean(centred * centred, axis=(0, 4), keepdims=True)
    return centred * lax.rsqrt(spread + norm_eps) * gain_rows[:, None, None, None, :]


def ordered_gains(gain_vector, quarter_order):
    gain_table = gain_vector.reshape(SPLITS, -1)
    selector = (quarter_order[:, None] == jnp.arange(SPLITS, dtype=jnp.int32)[None, :]).astype(
        jnp.float32
    )
    return jnp.dot(selector, gain_table, precision=lax.Precision.HIGHEST)


def plain_body(tokens, ln_gain, w_qkv, q_gain, k_gain):
    local_rows = tokens.shape[0]
    normed = layer_norm(tokens.astype(jnp.float32), ln_gain).astype(jnp.bfloat16)
    flat_weight = w_qkv.reshape(w_qkv.shape[0], -1)
    out_width = flat_weight.shape[1]
    row_piece = lax.all_gather(w_qkv, "dp", axis=0, tiled=True)
    partial_value = jnp.dot(
        normed, row_piece.reshape(row_piece.shape[0], out_width), preferred_element_type=jnp.float32
    )
    projected = partial_value.astype(jnp.bfloat16)
    groups = lax.axis_size("mp") // SPLITS
    head_count = HEADS // groups
    quarter_rows = PATCHES // SPLITS
    my_quarter = lax.axis_index("mp") // groups
    images = local_rows // PATCHES
    head_view = projected.reshape(images, PATCHES, 3, head_count, HEAD_DIM // SPLITS)
    queries = head_view[:, :, 0]
    keys_vals = head_view[:, :, 1:]
    counting = jnp.arange(SPLITS, dtype=jnp.int32)
    own_rows = lax.dynamic_slice_in_dim(queries, my_quarter * quarter_rows, quarter_rows, 1)
    query_list = [own_rows]
    pair_list = [keys_vals]
    for offset in range(1, SPLITS):
        outgoing = lax.dynamic_slice_in_dim(
            queries, (my_quarter + offset) % SPLITS * quarter_rows, quarter_rows, 1
        )
        got_query, got_pair = from_behind((outgoing, keys_vals), "mp", offset * groups)
        query_list.append(got_query)
        pair_list.append(got_pair)
    query_pieces = jnp.stack(query_list, 0)
    pair_pieces = jnp.stack(pair_list, 0)
    quarter_order = (my_quarter - counting) % SPLITS
    query_normed = (
        head_norm(query_pieces, ordered_gains(q_gain, quarter_order)) * HEAD_DIM ** (-0.5)
    ).astype(jnp.bfloat16)
    key_normed = head_norm(pair_pieces[:, :, :, 0], ordered_gains(k_gain, quarter_order)).astype(
        jnp.bfloat16
    )
    value_part = pair_pieces[:, :, :, 1]
    scores = jnp.einsum(
        "sirhe,sikhe->ihrk", query_normed, key_normed, preferred_element_type=jnp.float32
    )
    raised = jnp.exp(scores)
    weights = (raised / jnp.sum(raised, axis=-1, keepdims=True)).astype(jnp.bfloat16)
    context = jnp.einsum(
        "ihrk,sikhe->sirhe", weights, value_part, preferred_element_type=jnp.float32
    ).astype(jnp.bfloat16)
    rows_list = [context[0]]
    for offset in range(1, SPLITS):
        wanted = (my_quarter - offset) % SPLITS
        slot_index = jnp.sum(jnp.where(quarter_order == wanted, counting, 0))
        outgoing = lax.dynamic_index_in_dim(context, slot_index, 0, keepdims=False)
        rows_list.append(from_behind(outgoing, "mp", (SPLITS - offset) * groups))
    own_block = jnp.roll(jnp.concatenate(rows_list, 1), my_quarter * quarter_rows, axis=1)
    return own_block.reshape(local_rows, -1)

MESH = pl.DeviceIdType.MESH
VMEM_LIMIT = 62 * 1024 * 1024
BLOCK = 256
PIECES = 4
GROUPS = 2
UNITS = 9
CHUNKS = "abd"


def column_norm(values, gain):
    centre = jnp.mean(values, axis=0, keepdims=True)
    centred = values - centre
    spread = jnp.mean(centred * centred, axis=0, keepdims=True)
    return centred * lax.rsqrt(spread + norm_eps) * gain


def span(start, size):
    return pl.ds(pl.multiple_of(start, size), size)


def fused_kernel(
    token_hbm, gain_ref, weight_hbm, q_gain_ref, k_gain_ref, out_ref,
    work, weight, own, other, share, total, partial, pieces, returned,
    q_gain, k_gain, swap, got,
    token_in, weight_in, weight_out, weight_got, swap_out, swap_got,
    share_out, share_got, relay_out, relay_got, partial_out, partial_got,
    piece_out, piece_got, context_out, context_got,
):
    scope = jax.named_scope
    dp, mp = lax.axis_index("dp"), lax.axis_index("mp")
    side, core = dp // 2, dp % 2
    quarter, group = mp // GROUPS, mp % GROUPS
    rows, features = token_hbm.shape
    depth, width = weight_hbm.shape[1:]
    half = features // 2
    images = rows // PATCHES
    part = HEAD_DIM // SPLITS
    quad_rows = PATCHES // 4
    piece_rows = quad_rows // PIECES
    small = BLOCK // SPLITS
    folded = depth // 2
    piece_lane = UNITS * BLOCK
    context_lane = 2 * piece_lane

    sibling = (side * 2 + 1 - core, mp)
    across = ((1 - side) * 2 + core, mp)
    near_group = (dp, quarter * GROUPS + 1 - group)
    near_quarter = (dp, (quarter + 1 - 2 * (quarter % 2)) * GROUPS + group)
    quad_place = (quarter % 2) * 2 + group
    near_place = (1 - quarter % 2) * 2 + group

    def quarter_at(offset):
        return (dp, (quarter + offset) % SPLITS * GROUPS + group)

    def remote(source, target, send, receive, device):
        return pltpu.make_async_remote_copy(
            src_ref=source, dst_ref=target, send_sem=send, recv_sem=receive,
            device_id=device, device_id_type=MESH,
        )

    def lines_of(image):
        return slice(image * PATCHES, (image + 1) * PATCHES)

    def token_load(image):
        lines = lines_of(image)
        return pltpu.make_async_copy(token_hbm.at[lines], work.at[lines], token_in.at[image])

    mine = span(core * depth, depth)

    def block_lanes(block):
        return slice(block * BLOCK, (block + 1) * BLOCK)

    def weight_load(block):
        columns = block_lanes(block)
        return pltpu.make_async_copy(
            weight_hbm.at[:, :, columns], weight.at[:, mine, columns], weight_in.at[block]
        )

    def weight_send(block):
        columns = block_lanes(block)
        return remote(
            weight_hbm.at[:, :, columns], weight.at[:, mine, columns],
            weight_out, weight_got.at[block], sibling,
        )

    inner = (quarter == 1) | (quarter == 2)
    partner = 3 - quarter

    def units_of(block):
        return slice(block * 3, block * 3 + 3)

    def swap_send(block):
        view = units_of(block)
        return remote(
            swap.at[view], got.at[0, view], swap_out, swap_got.at[block],
            (dp, partner * GROUPS + group),
        )

    def swap_pass(block):
        view = units_of(block)
        return remote(
            got.at[0, view], got.at[1, view],
            swap_out, swap_got.at[3 + block], sibling,
        )

    def swap_lanes(block, here):
        first = block * BLOCK + (2 * small if here == 1 else 0)
        return slice(first, first + 2 * small)

    def swap_fold():
        for here, side in ((1, 0), (2, 1)):
            @pl.when(quarter == here)
            def _(here=here, side=side):
                for unit in range(UNITS):
                    block, kind = divmod(unit, 3)
                    lanes = swap_lanes(block, here)
                    swap[unit] = jnp.concatenate(
                        [
                            weight[kind, span(core * depth + row * folded, folded), lanes][
                                :, side * small : (side + 1) * small
                            ]
                            for row in range(2)
                        ],
                        axis=1,
                    )

    def swap_unfold(block, slot):
        owner = core if slot == 0 else 1 - core
        for here, side in ((1, 0), (2, 1)):
            @pl.when(quarter == here)
            def _(here=here, side=side):
                for kind in range(3):
                    lanes = swap_lanes(block, here)
                    for row in range(2):
                        lines = span(owner * depth + row * folded, folded)
                        fresh = got[slot, block * 3 + kind][:, row * small : (row + 1) * small]
                        held = weight[kind, lines, lanes][
                            :, (1 - side) * small : (2 - side) * small
                        ]
                        both = (fresh, held) if side == 0 else (held, fresh)
                        weight[kind, lines, lanes] = jnp.concatenate(both, axis=1)

    def swap_arrive(block):
        with scope("w_swap"):
            weight_send(block).wait_recv()

            @pl.when(inner)
            def _():
                swap_send(block).wait_recv()
                swap_pass(block).start()

    def swap_finish(block):
        with scope("swap_finish"):
            @pl.when(inner)
            def _():
                swap_unfold(block, 0)
                swap_pass(block).wait_recv()
                swap_unfold(block, 1)

    def unless_swapped(offset, action):
        if offset == 2:
            action()
        else:
            pl.when(quarter != (1 if offset == 1 else 2))(action)

    def quad_view(image, place, piece=None):
        line = image * PATCHES + place * quad_rows
        if piece is None:
            return other.at[span(line, quad_rows)]
        return other.at[span(line + piece * piece_rows, piece_rows)]

    def share_slot(image, piece):
        return piece if piece is not None else PIECES + image - 1

    def share_send(image, piece=None):
        if piece is None:
            source = share.at[image * quad_rows : (image + 1) * quad_rows]
        else:
            source = share.at[span(image * quad_rows + piece * piece_rows, piece_rows)]
        slot = share_slot(image, piece)
        return remote(
            source, quad_view(image, quad_place, piece),
            share_out, share_got.at[slot], across,
        )

    def relay(image, way, piece=None):
        places = (quad_place, quad_place, near_place, quad_place + 1 - 2 * group)
        view = quad_view(image, places[way], piece)
        slot = share_slot(image, piece) * 4 + way
        device = near_group if way in (1, 2) else near_quarter
        return remote(view, view, relay_out, relay_got.at[slot], device)

    def parts_of(image, chunk):
        first = CHUNKS.index(chunk) * 3
        if (image, chunk) == (0, "a"):
            return [(unit, 1) for unit in range(first, first + 3)]
        return [(first, 3)]

    def chunk_slot(image, chunk, step):
        if image == 0:
            return step if chunk == "a" else 2 + CHUNKS.index(chunk)
        return 2 + image * 3 + CHUNKS.index(chunk)

    def partial_send(image, chunk, step):
        first, count = parts_of(image, chunk)[step]
        columns = slice(first * BLOCK, (first + count) * BLOCK)
        slot = chunk_slot(image, chunk, step)
        return remote(
            work.at[lines_of(image), columns], partial.at[image, :, columns],
            partial_out, partial_got.at[slot], across,
        )

    def piece_view(image, target, first, count):
        lane = piece_lane + first * BLOCK
        return work.at[
            span(image * PATCHES + target * small, small), slice(lane, lane + count * BLOCK)
        ]

    def piece_send(image, chunk, step, offset):
        first, count = parts_of(image, chunk)[step]
        slot = chunk_slot(image, chunk, step)
        return remote(
            piece_view(image, (quarter + offset) % SPLITS, first, count),
            pieces.at[image, quarter, :, first * BLOCK : (first + count) * BLOCK],
            piece_out, piece_got.at[slot], quarter_at(offset),
        )

    def context_view(image, chunk, target):
        lane = context_lane + CHUNKS.index(chunk) * BLOCK
        return work.at[span(image * PATCHES + target * small, small), slice(lane, lane + BLOCK)]

    def context_send(image, chunk, offset):
        slot = image * 3 + CHUNKS.index(chunk)
        return remote(
            context_view(image, chunk, (quarter + offset) % SPLITS),
            returned.at[image, CHUNKS.index(chunk), quarter],
            context_out, context_got.at[slot], quarter_at(offset),
        )

    own_half = span(side * half, half)
    other_half = span((1 - side) * half, half)

    def normalize(line, count, share_line=None):
        lines = span(line, count)
        values = work[lines, :].astype(jnp.float32)
        centre = jnp.mean(values, axis=-1, keepdims=True)
        centred = values - centre
        spread = jnp.mean(centred * centred, axis=-1, keepdims=True)
        scale = lax.rsqrt(spread + norm_eps)

        def scaled(columns):
            return (
                (work[lines, columns].astype(jnp.float32) - centre) * scale * gain_ref[:, columns]
            ).astype(jnp.bfloat16)

        if share_line is not None:
            share[span(share_line, count), :] = scaled(other_half)
        own[lines, :] = scaled(own_half)

    def own_part(block, step):
        with scope("own_part"):
            total[:, span((block * 3 + step) * BLOCK, BLOCK)] = jnp.dot(
                own[...], weight[step, :, block_lanes(block)], preferred_element_type=jnp.float32
            )

    def own_chunk(chunk):
        def looped(step, carry):
            own_part(CHUNKS.index(chunk), step)
            return carry

        lax.fori_loop(0, 3, looped, 0)

    def send_partial(image, chunk):
        block = CHUNKS.index(chunk)
        split = len(parts_of(image, chunk)) > 1

        def other_part(step):
            work[lines_of(image), span((block * 3 + step) * BLOCK, BLOCK)] = jnp.dot(
                other[lines_of(image), :], weight[step, :, block_lanes(block)],
                preferred_element_type=jnp.float32,
            ).astype(jnp.bfloat16)

        def looped(step, carry):
            other_part(step)
            return carry

        with scope(f"other_part_{image}{chunk}"):
            if split:
                for step in range(3):
                    other_part(step)
                    partial_send(image, chunk, step).start()
            else:
                lax.fori_loop(0, 3, looped, 0)
                partial_send(image, chunk, 0).start()

    def sum_step(image, chunk, step):
        first, count = parts_of(image, chunk)[step]
        with scope(f"w_partial_{image}{chunk}"):
            partial_send(image, chunk, step).wait_recv()
        for unit in range(first, first + count):
            columns = slice(unit * BLOCK, (unit + 1) * BLOCK)
            whole = total[lines_of(image), columns] + partial[image, :, columns].astype(
                jnp.float32
            )
            work[
                lines_of(image), piece_lane + unit * BLOCK : piece_lane + (unit + 1) * BLOCK
            ] = whole.T.astype(jnp.bfloat16)
        for offset in (2, 1, 3):
            unless_swapped(
                offset, lambda offset=offset: piece_send(image, chunk, step, offset).start()
            )

    def sum_up(image, chunk):
        for step in range(len(parts_of(image, chunk))):
            sum_step(image, chunk, step)
        first = CHUNKS.index(chunk) * 3
        lanes = slice(first * BLOCK, (first + 3) * BLOCK)
        pieces[image, quarter, :, lanes] = piece_view(image, quarter, first, 3)[...]

        @pl.when(inner)
        def _():
            pieces[image, partner, :, lanes] = piece_view(image, partner, first, 3)[...]

    def attend(image, chunk):
        with scope(f"w_piece_{image}{chunk}"):
            for step, (first, count) in enumerate(parts_of(image, chunk)):
                slot = chunk_slot(image, chunk, step)
                lanes = slice(first * BLOCK, (first + count) * BLOCK)
                for number, condition in ((2, inner), (3, jnp.logical_not(inner))):
                    @pl.when(condition)
                    def _(number=number, slot=slot, lanes=lanes):
                        view = pieces.at[image, :number, :, lanes]
                        remote(
                            view, view, piece_out, piece_got.at[slot], quarter_at(1)
                        ).wait_recv()

        def gathered(head, kind):
            lane = (CHUNKS.index(chunk) * 3 + kind) * BLOCK
            lines = slice(head * part, (head + 1) * part)
            found = [pieces[image, source, lines, lane : lane + BLOCK] for source in range(SPLITS)]
            return jnp.concatenate(found, axis=0)

        with scope(f"attend_{image}{chunk}"):
            for head in range(small // part):
                query = (
                    column_norm(gathered(head, 0).astype(jnp.float32), q_gain[...])
                    * HEAD_DIM ** (-0.5)
                ).astype(jnp.bfloat16)
                key = column_norm(gathered(head, 1).astype(jnp.float32), k_gain[...]).astype(
                    jnp.bfloat16
                )
                scores = lax.dot_general(
                    key, query, (((0,), (0,)), ((), ())), preferred_element_type=jnp.float32
                )
                raised = jnp.exp(scores)
                weights = (raised / jnp.sum(raised, axis=0, keepdims=True)).astype(jnp.bfloat16)
                attended = jnp.dot(
                    gathered(head, 2), weights, preferred_element_type=jnp.float32
                ).astype(jnp.bfloat16)
                lane = context_lane + CHUNKS.index(chunk) * BLOCK
                for target in range(SPLITS):
                    line = image * PATCHES + target * small + head * part
                    work[line : line + part, lane : lane + BLOCK] = attended[
                        target * part : (target + 1) * part
                    ]
        for offset in (2, 1, 3):
            context_send(image, chunk, offset).start()
        returned[image, CHUNKS.index(chunk), quarter] = context_view(image, chunk, quarter)[...]

    def store(image, chunk):
        block = CHUNKS.index(chunk)
        with scope(f"w_context_{image}{chunk}"):
            view = returned.at[image, block, : SPLITS - 1]
            remote(
                view, view, context_out, context_got.at[image * 3 + block], quarter_at(1)
            ).wait_recv()
        out_ref[lines_of(image), block * BLOCK : (block + 1) * BLOCK] = (
            returned[image, block].reshape(BLOCK, PATCHES).T
        )

    def token_ready(image):
        with scope(f"w_token_{image}"):
            if image == 0:
                for piece in range(PIECES):
                    if piece < PIECES // 2:
                        relay(image, 1, piece).wait_recv()
                        relay(image, 2, piece).wait_recv()
                    else:
                        relay(image, 0, piece).wait_recv()
                        relay(image, 3, piece).wait_recv()
            else:
                relay(image, 1).wait_recv()
                relay(image, 2).wait_recv()

    def pass_quarter(image, piece=None):
        with scope(f"w_share_{image}"):
            share_send(image, piece).wait_recv()
        relay(image, 0, piece).start()

    def pass_group(image, piece=None):
        relay(image, 1, piece).start()

    def pass_near(image, piece=None):
        with scope(f"w_near_{image}"):
            relay(image, 0, piece).wait_recv()
        relay(image, 2, piece).start()

    def pass_side(image, piece):
        with scope(f"w_side_{image}"):
            relay(image, 1, piece).wait_recv()
        relay(image, 3, piece).start()

    def drain(view, semaphore):
        remote(view, view, semaphore, weight_got.at[0], sibling).wait_send()

    barrier = pltpu.get_barrier_semaphore()
    partners = [sibling, across, near_group] + [quarter_at(o) for o in range(1, SPLITS)]
    for device in partners:
        pl.semaphore_signal(barrier, inc=1, device_id=device, device_id_type=MESH)
    token_load(0).start()
    for block in range(3):
        weight_load(block).start()
    for image in range(1, images):
        token_load(image).start()
    q_gain[...] = jnp.broadcast_to(q_gain_ref[...], (PATCHES, HEAD_DIM)).T
    k_gain[...] = jnp.broadcast_to(k_gain_ref[...], (PATCHES, HEAD_DIM)).T

    def share_norm(image, carry):
        normalize(image * PATCHES + quad_place * quad_rows, quad_rows, image * quad_rows)
        return carry

    token_load(0).wait()
    with scope("norm_share_0"):
        share_norm(0, 0)
    with scope("barrier"):
        pl.semaphore_wait(barrier, len(partners))
    for piece in range(PIECES):
        share_send(0, piece).start()
    weight_send(0).start()
    for block in range(3):
        weight_load(block).wait()
    with scope("fold"):
        swap_fold()

    @pl.when(inner)
    def _():
        for block in range(3):
            swap_send(block).start()

    token_load(1).wait()
    token_load(2).wait()
    with scope("norm_share"):
        lax.fori_loop(1, images, share_norm, 0)
    for image in range(1, images):
        share_send(image).start()
    weight_send(1).start()
    weight_send(2).start()

    def rest_norm(image, step, carry):
        normalize(image * PATCHES + (quad_place + step + 1) % 4 * quad_rows, quad_rows)
        return carry

    def rest_image(image, carry):
        with scope("norm_rest"):
            lax.fori_loop(0, 3, functools.partial(rest_norm, image), 0)

        @pl.when(image > 0)
        def _():
            pass_quarter(0, image - 1)
            pass_group(0, image - 1)

        return carry

    lax.fori_loop(0, images, rest_image, 0)
    pass_quarter(0, 2)
    pass_group(0, 2)
    pass_quarter(0, 3)
    pass_group(0, 3)
    pass_near(0, 0)
    pass_near(0, 1)
    swap_arrive(0)
    pass_side(0, 2)
    pass_side(0, 3)
    swap_finish(0)
    pass_quarter(1)
    pass_group(1)
    own_chunk("a")
    token_ready(0)
    send_partial(0, "a")
    swap_arrive(1)
    swap_finish(1)
    send_partial(0, "b")
    pass_quarter(2)
    sum_up(0, "a")
    own_chunk("b")
    pass_near(1)
    pass_group(2)
    swap_arrive(2)
    swap_finish(2)
    send_partial(0, "d")
    sum_up(0, "b")
    own_chunk("d")
    token_ready(1)
    send_partial(1, "a")
    send_partial(1, "b")
    send_partial(1, "d")
    attend(0, "a")
    sum_up(0, "d")
    pass_near(2)
    sum_up(1, "a")
    token_ready(2)
    send_partial(2, "a")
    send_partial(2, "b")
    send_partial(2, "d")
    attend(0, "b")
    sum_up(1, "b")
    attend(0, "d")
    sum_up(1, "d")
    attend(1, "a")
    sum_up(2, "a")
    attend(1, "b")
    sum_up(2, "b")
    attend(1, "d")
    sum_up(2, "d")
    attend(2, "a")
    for chunk in CHUNKS:
        store(0, chunk)
    store(1, "a")
    attend(2, "b")
    store(1, "b")
    attend(2, "d")
    store(1, "d")
    for chunk in CHUNKS:
        store(2, chunk)

    drain(weight.at[:, mine, :], weight_out)
    drain(share, share_out)
    drain(other.at[: images * 3 * quad_rows], relay_out)
    drain(work.at[:, :piece_lane], partial_out)
    drain(work.at[: images * small, :piece_lane], context_out)

    @pl.when(inner)
    def _():
        drain(got, swap_out)
        drain(work.at[: images * 2 * small, :piece_lane], piece_out)

    @pl.when(jnp.logical_not(inner))
    def _():
        drain(work.at[: images * 3 * small, :piece_lane], piece_out)


def fused(tokens, gain, weights, q_gain, k_gain):
    rows, features = tokens.shape
    kinds, depth, width = weights.shape
    images = rows // PATCHES
    small = BLOCK // SPLITS
    whole = pl.BlockSpec(memory_space=pltpu.VMEM)
    outside = pl.BlockSpec(memory_space=pl.ANY)
    dma = pltpu.SemaphoreType.DMA

    def vmem(*shape, dtype=jnp.bfloat16):
        return pltpu.VMEM(shape, dtype)

    share_count = PIECES + images - 1
    chunk_count = images * 3 + 2
    return pl.pallas_call(
        fused_kernel,
        out_shape=jax.ShapeDtypeStruct((rows, width), jnp.bfloat16),
        in_specs=[outside, whole, outside, whole, whole],
        out_specs=whole,
        scratch_shapes=[
            vmem(rows, features),
            vmem(kinds, 2 * depth, width),
            vmem(rows, features // 2),
            vmem(rows, features // 2),
            vmem(images * PATCHES // 4, features // 2),
            vmem(rows, kinds * width, dtype=jnp.float32),
            vmem(images, PATCHES, kinds * width),
            vmem(images, SPLITS, small, UNITS * PATCHES),
            vmem(images, 3, SPLITS, small, PATCHES),
            vmem(HEAD_DIM, PATCHES, dtype=jnp.float32),
            vmem(HEAD_DIM, PATCHES, dtype=jnp.float32),
            vmem(UNITS, depth // 2, 2 * small),
            vmem(2, UNITS, depth // 2, 2 * small),
            dma((images,)), dma((3,)), dma, dma((3,)),
            dma, dma((6,)),
            dma, dma((share_count,)),
            dma, dma((4 * share_count,)),
            dma, dma((chunk_count,)),
            dma, dma((chunk_count,)),
            dma, dma((images * 3,)),
        ],
        compiler_params=pltpu.CompilerParams(
            collective_id=0, has_side_effects=True, vmem_limit_bytes=VMEM_LIMIT
        ),
        name="fused",
    )(tokens, gain.reshape(1, features), weights, q_gain.reshape(1, HEAD_DIM),
      k_gain.reshape(1, HEAD_DIM))


def body(tokens, ln_gain, w_qkv, q_gain, k_gain):
    fits = lax.axis_size("dp") == 4 and lax.axis_size("mp") == GROUPS * SPLITS
    fits = fits and tokens.shape == (3 * PATCHES, 4 * w_qkv.shape[0])
    fits = fits and w_qkv.shape[1:] == (3, 3 * BLOCK) and w_qkv.shape[0] % BLOCK == 0
    if not fits:
        return plain_body(tokens, ln_gain, w_qkv, q_gain, k_gain)
    return fused(tokens, ln_gain, jnp.transpose(w_qkv, (1, 0, 2)), q_gain, k_gain)


def solution(mesh):
    return jax.shard_map(
        body,
        mesh=mesh,
        in_specs=(P("dp", None), P(), P("dp", None, "mp"), P(), P()),
        out_specs=P("dp", "mp"),
        check_vma=False,
    )
```

```python
import functools

import jax
import jax.numpy as jnp
from jax import lax
from jax.experimental import pallas as pl
from jax.experimental.pallas import tpu as pltpu
from jax.sharding import PartitionSpec as P


HEADS = 48
HEAD_DIM = 128
PATCHES = 256
SPLITS = 4


norm_eps = 1e-06


def from_behind(shard, axis, by):
    length = lax.axis_size(axis)
    return lax.ppermute(shard, axis, [(i, (i + by) % length) for i in range(length)])


def layer_norm(values, gain_vector):
    centre = jnp.mean(values, axis=-1, keepdims=True)
    centred = values - centre
    spread = jnp.mean(centred * centred, axis=-1, keepdims=True)
    return centred * lax.rsqrt(spread + norm_eps) * gain_vector


def head_norm(pieces, gain_rows):
    values = pieces.astype(jnp.float32)
    centre = jnp.mean(values, axis=(0, 4), keepdims=True)
    centred = values - centre
    spread = jnp.mean(centred * centred, axis=(0, 4), keepdims=True)
    return centred * lax.rsqrt(spread + norm_eps) * gain_rows[:, None, None, None, :]


def ordered_gains(gain_vector, quarter_order):
    gain_table = gain_vector.reshape(SPLITS, -1)
    selector = (quarter_order[:, None] == jnp.arange(SPLITS, dtype=jnp.int32)[None, :]).astype(
        jnp.float32
    )
    return jnp.dot(selector, gain_table, precision=lax.Precision.HIGHEST)


def plain_body(tokens, ln_gain, w_qkv, q_gain, k_gain):
    local_rows = tokens.shape[0]
    normed = layer_norm(tokens.astype(jnp.float32), ln_gain).astype(jnp.bfloat16)
    flat_weight = w_qkv.reshape(w_qkv.shape[0], -1)
    out_width = flat_weight.shape[1]
    row_piece = lax.all_gather(w_qkv, "dp", axis=0, tiled=True)
    partial_value = jnp.dot(
        normed, row_piece.reshape(row_piece.shape[0], out_width), preferred_element_type=jnp.float32
    )
    projected = partial_value.astype(jnp.bfloat16)
    groups = lax.axis_size("mp") // SPLITS
    head_count = HEADS // groups
    quarter_rows = PATCHES // SPLITS
    my_quarter = lax.axis_index("mp") // groups
    images = local_rows // PATCHES
    head_view = projected.reshape(images, PATCHES, 3, head_count, HEAD_DIM // SPLITS)
    queries = head_view[:, :, 0]
    keys_vals = head_view[:, :, 1:]
    counting = jnp.arange(SPLITS, dtype=jnp.int32)
    own_rows = lax.dynamic_slice_in_dim(queries, my_quarter * quarter_rows, quarter_rows, 1)
    query_list = [own_rows]
    pair_list = [keys_vals]
    for offset in range(1, SPLITS):
        outgoing = lax.dynamic_slice_in_dim(
            queries, (my_quarter + offset) % SPLITS * quarter_rows, quarter_rows, 1
        )
        got_query, got_pair = from_behind((outgoing, keys_vals), "mp", offset * groups)
        query_list.append(got_query)
        pair_list.append(got_pair)
    query_pieces = jnp.stack(query_list, 0)
    pair_pieces = jnp.stack(pair_list, 0)
    quarter_order = (my_quarter - counting) % SPLITS
    query_normed = (
        head_norm(query_pieces, ordered_gains(q_gain, quarter_order)) * HEAD_DIM ** (-0.5)
    ).astype(jnp.bfloat16)
    key_normed = head_norm(pair_pieces[:, :, :, 0], ordered_gains(k_gain, quarter_order)).astype(
        jnp.bfloat16
    )
    value_part = pair_pieces[:, :, :, 1]
    scores = jnp.einsum(
        "sirhe,sikhe->ihrk", query_normed, key_normed, preferred_element_type=jnp.float32
    )
    raised = jnp.exp(scores)
    weights = (raised / jnp.sum(raised, axis=-1, keepdims=True)).astype(jnp.bfloat16)
    context = jnp.einsum(
        "ihrk,sikhe->sirhe", weights, value_part, preferred_element_type=jnp.float32
    ).astype(jnp.bfloat16)
    rows_list = [context[0]]
    for offset in range(1, SPLITS):
        wanted = (my_quarter - offset) % SPLITS
        slot_index = jnp.sum(jnp.where(quarter_order == wanted, counting, 0))
        outgoing = lax.dynamic_index_in_dim(context, slot_index, 0, keepdims=False)
        rows_list.append(from_behind(outgoing, "mp", (SPLITS - offset) * groups))
    own_block = jnp.roll(jnp.concatenate(rows_list, 1), my_quarter * quarter_rows, axis=1)
    return own_block.reshape(local_rows, -1)

MESH = pl.DeviceIdType.MESH
VMEM_LIMIT = 62 * 1024 * 1024
BLOCK = 256
PIECES = 4
GROUPS = 2
UNITS = 9
CHUNKS = "abd"
SWAPPED = "abd"


def column_norm(values, gain):
    centre = jnp.mean(values, axis=0, keepdims=True)
    centred = values - centre
    spread = jnp.mean(centred * centred, axis=0, keepdims=True)
    return centred * lax.rsqrt(spread + norm_eps) * gain


def span(start, size):
    return pl.ds(pl.multiple_of(start, size), size)


def fused_kernel(
    token_hbm, gain_ref, weight_hbm, q_gain_ref, k_gain_ref, out_ref,
    work, weight, own, other, share, total, partial, pieces, returned,
    q_gain, k_gain, swap, got,
    token_in, weight_in, weight_out, weight_got, swap_out, swap_got,
    share_out, share_got, relay_out, relay_got, partial_out, partial_got,
    piece_out, piece_got, context_out, context_got,
):
    scope = jax.named_scope
    dp, mp = lax.axis_index("dp"), lax.axis_index("mp")
    side, core = dp // 2, dp % 2
    quarter, group = mp // GROUPS, mp % GROUPS
    rows, features = token_hbm.shape
    depth, width = weight_hbm.shape[1:]
    half = features // 2
    images = rows // PATCHES
    part = HEAD_DIM // SPLITS
    quad_rows = PATCHES // 4
    piece_rows = quad_rows // PIECES
    small = BLOCK // SPLITS
    folded = depth // 2
    piece_lane = UNITS * BLOCK
    context_lane = 2 * piece_lane

    sibling = (side * 2 + 1 - core, mp)
    across = ((1 - side) * 2 + core, mp)
    near_group = (dp, quarter * GROUPS + 1 - group)
    near_quarter = (dp, (quarter + 1 - 2 * (quarter % 2)) * GROUPS + group)
    quad_place = (quarter % 2) * 2 + group
    near_place = (1 - quarter % 2) * 2 + group

    def quarter_at(offset):
        return (dp, (quarter + offset) % SPLITS * GROUPS + group)

    def remote(source, target, send, receive, device):
        return pltpu.make_async_remote_copy(
            src_ref=source, dst_ref=target, send_sem=send, recv_sem=receive,
            device_id=device, device_id_type=MESH,
        )

    def lines_of(image):
        return slice(image * PATCHES, (image + 1) * PATCHES)

    def token_load(image):
        lines = lines_of(image)
        return pltpu.make_async_copy(token_hbm.at[lines], work.at[lines], token_in.at[image])

    def quarter_load(turn, semaphore):
        lines = span((quad_place + turn) % 4 * quad_rows, quad_rows)
        return pltpu.make_async_copy(token_hbm.at[lines], work.at[lines], semaphore)

    def first_load():
        return quarter_load(0, token_in.at[0])

    def rest_load(turn):
        return quarter_load(turn, token_in.at[3])

    def rest_wait():
        lines = slice(0, 3 * quad_rows)
        pltpu.make_async_copy(token_hbm.at[lines], work.at[lines], token_in.at[3]).wait()

    mine = span(core * depth, depth)

    def block_lanes(block):
        return slice(block * BLOCK, (block + 1) * BLOCK)

    def weight_load(block):
        columns = block_lanes(block)
        return pltpu.make_async_copy(
            weight_hbm.at[:, :, columns], weight.at[:, mine, columns], weight_in.at[block]
        )

    def weight_send(block):
        columns = block_lanes(block)
        return remote(
            weight_hbm.at[:, :, columns], weight.at[:, mine, columns],
            weight_out, weight_got.at[block], sibling,
        )

    inner = (quarter == 1) | (quarter == 2)
    partner = 3 - quarter

    def units_of(block):
        return slice(block * 3, block * 3 + 3)

    def swap_send(block):
        view = units_of(block)
        return remote(
            swap.at[view], got.at[0, view], swap_out, swap_got.at[block],
            (dp, partner * GROUPS + group),
        )

    def swap_pass(block):
        view = units_of(block)
        return remote(
            got.at[0, view], got.at[1, view],
            swap_out, swap_got.at[3 + block], sibling,
        )

    def swap_lanes(block, here):
        first = block * BLOCK + (2 * small if here == 1 else 0)
        return slice(first, first + 2 * small)

    def swap_fold():
        for here, side in ((1, 0), (2, 1)):
            @pl.when(quarter == here)
            def _(here=here, side=side):
                for unit in range(3 * len(SWAPPED)):
                    block, kind = divmod(unit, 3)
                    lanes = swap_lanes(block, here)
                    swap[unit] = jnp.concatenate(
                        [
                            weight[kind, span(core * depth + row * folded, folded), lanes][
                                :, side * small : (side + 1) * small
                            ]
                            for row in range(2)
                        ],
                        axis=1,
                    )

    def swap_unfold(block, slot):
        owner = core if slot == 0 else 1 - core
        for here, side in ((1, 0), (2, 1)):
            @pl.when(quarter == here)
            def _(here=here, side=side):
                for kind in range(3):
                    lanes = swap_lanes(block, here)
                    for row in range(2):
                        lines = span(owner * depth + row * folded, folded)
                        fresh = got[slot, block * 3 + kind][:, row * small : (row + 1) * small]
                        held = weight[kind, lines, lanes][
                            :, (1 - side) * small : (2 - side) * small
                        ]
                        both = (fresh, held) if side == 0 else (held, fresh)
                        weight[kind, lines, lanes] = jnp.concatenate(both, axis=1)

    def swap_arrive(block):
        if block >= len(SWAPPED):
            weight_send(block).wait_recv()
            return
        with scope("w_swap"):
            weight_send(block).wait_recv()

            @pl.when(inner)
            def _():
                swap_send(block).wait_recv()
                swap_pass(block).start()

    def swap_finish(block):
        if block >= len(SWAPPED):
            return
        with scope("swap_finish"):
            @pl.when(inner)
            def _():
                swap_unfold(block, 0)
                swap_pass(block).wait_recv()
                swap_unfold(block, 1)

    def unless_swapped(chunk, offset, action):
        if offset == 2 or chunk not in SWAPPED:
            action()
        else:
            pl.when(quarter != (1 if offset == 1 else 2))(action)

    def quad_view(image, place, piece=None):
        line = image * PATCHES + place * quad_rows
        if piece is None:
            return other.at[span(line, quad_rows)]
        return other.at[span(line + piece * piece_rows, piece_rows)]

    def share_slot(image, piece):
        return piece if piece is not None else PIECES + image - 1

    def share_send(image, piece=None):
        if piece is None:
            source = share.at[image * quad_rows : (image + 1) * quad_rows]
        else:
            source = share.at[span(image * quad_rows + piece * piece_rows, piece_rows)]
        slot = share_slot(image, piece)
        return remote(
            source, quad_view(image, quad_place, piece),
            share_out, share_got.at[slot], across,
        )

    def relay(image, way, piece=None):
        places = (quad_place, quad_place, near_place, quad_place + 1 - 2 * group)
        view = quad_view(image, places[way], piece)
        slot = share_slot(image, piece) * 4 + way
        device = near_group if way in (1, 2) else near_quarter
        return remote(view, view, relay_out, relay_got.at[slot], device)

    def parts_of(image, chunk):
        first = CHUNKS.index(chunk) * 3
        if (image, chunk) == (0, "a"):
            return [(unit, 1) for unit in range(first, first + 3)]
        return [(first, 3)]

    def chunk_slot(image, chunk, step):
        if image == 0:
            return step if chunk == "a" else 2 + CHUNKS.index(chunk)
        return 2 + image * 3 + CHUNKS.index(chunk)

    def partial_send(image, chunk, step):
        first, count = parts_of(image, chunk)[step]
        columns = slice(first * BLOCK, (first + count) * BLOCK)
        slot = chunk_slot(image, chunk, step)
        return remote(
            work.at[lines_of(image), columns], partial.at[image, :, columns],
            partial_out, partial_got.at[slot], across,
        )

    def piece_view(image, target, first, count):
        lane = piece_lane + first * BLOCK
        return work.at[
            span(image * PATCHES + target * small, small), slice(lane, lane + count * BLOCK)
        ]

    def piece_send(image, chunk, step, offset):
        first, count = parts_of(image, chunk)[step]
        slot = chunk_slot(image, chunk, step)
        return remote(
            piece_view(image, (quarter + offset) % SPLITS, first, count),
            pieces.at[image, quarter, :, first * BLOCK : (first + count) * BLOCK],
            piece_out, piece_got.at[slot], quarter_at(offset),
        )

    def context_view(image, chunk, target):
        lane = context_lane + CHUNKS.index(chunk) * BLOCK
        return work.at[span(image * PATCHES + target * small, small), slice(lane, lane + BLOCK)]

    def context_send(image, chunk, offset):
        slot = image * 3 + CHUNKS.index(chunk)
        return remote(
            context_view(image, chunk, (quarter + offset) % SPLITS),
            returned.at[image, CHUNKS.index(chunk), quarter],
            context_out, context_got.at[slot], quarter_at(offset),
        )

    own_half = span(side * half, half)
    other_half = span((1 - side) * half, half)

    def normalize(line, count, share_line=None):
        lines = span(line, count)
        values = work[lines, :].astype(jnp.float32)
        centre = jnp.mean(values, axis=-1, keepdims=True)
        centred = values - centre
        spread = jnp.mean(centred * centred, axis=-1, keepdims=True)
        scale = lax.rsqrt(spread + norm_eps)

        def scaled(columns):
            return (
                (work[lines, columns].astype(jnp.float32) - centre) * scale * gain_ref[:, columns]
            ).astype(jnp.bfloat16)

        if share_line is not None:
            share[span(share_line, count), :] = scaled(other_half)
        own[lines, :] = scaled(own_half)

    def own_part(block, step):
        with scope("own_part"):
            total[:, span((block * 3 + step) * BLOCK, BLOCK)] = jnp.dot(
                own[...], weight[step, :, block_lanes(block)], preferred_element_type=jnp.float32
            )

    def own_chunk(chunk):
        def looped(step, carry):
            own_part(CHUNKS.index(chunk), step)
            return carry

        lax.fori_loop(0, 3, looped, 0)

    def send_partial(image, chunk):
        block = CHUNKS.index(chunk)
        split = len(parts_of(image, chunk)) > 1

        def other_part(step):
            work[lines_of(image), span((block * 3 + step) * BLOCK, BLOCK)] = jnp.dot(
                other[lines_of(image), :], weight[step, :, block_lanes(block)],
                preferred_element_type=jnp.float32,
            ).astype(jnp.bfloat16)

        def looped(step, carry):
            other_part(step)
            return carry

        with scope(f"other_part_{image}{chunk}"):
            if split:
                for step in range(3):
                    other_part(step)
                    partial_send(image, chunk, step).start()
            else:
                lax.fori_loop(0, 3, looped, 0)
                partial_send(image, chunk, 0).start()

    def sum_step(image, chunk, step):
        first, count = parts_of(image, chunk)[step]
        with scope(f"w_partial_{image}{chunk}"):
            partial_send(image, chunk, step).wait_recv()
        for unit in range(first, first + count):
            columns = slice(unit * BLOCK, (unit + 1) * BLOCK)
            whole = total[lines_of(image), columns] + partial[image, :, columns].astype(
                jnp.float32
            )
            work[
                lines_of(image), piece_lane + unit * BLOCK : piece_lane + (unit + 1) * BLOCK
            ] = whole.T.astype(jnp.bfloat16)
        for offset in (2, 1, 3):
            unless_swapped(
                chunk, offset, lambda offset=offset: piece_send(image, chunk, step, offset).start()
            )

    def sum_up(image, chunk):
        for step in range(len(parts_of(image, chunk))):
            sum_step(image, chunk, step)
        sum_keep(image, chunk)

    def sum_keep(image, chunk):
        first = CHUNKS.index(chunk) * 3
        lanes = slice(first * BLOCK, (first + 3) * BLOCK)
        pieces[image, quarter, :, lanes] = piece_view(image, quarter, first, 3)[...]

        if chunk in SWAPPED:
            @pl.when(inner)
            def _():
                pieces[image, partner, :, lanes] = piece_view(image, partner, first, 3)[...]

    def attend(image, chunk):
        with scope(f"w_piece_{image}{chunk}"):
            for step, (first, count) in enumerate(parts_of(image, chunk)):
                slot = chunk_slot(image, chunk, step)
                lanes = slice(first * BLOCK, (first + count) * BLOCK)

                def wait_for(number, slot=slot, lanes=lanes):
                    view = pieces.at[image, :number, :, lanes]
                    remote(view, view, piece_out, piece_got.at[slot], quarter_at(1)).wait_recv()

                if chunk in SWAPPED:
                    pl.when(inner)(functools.partial(wait_for, SPLITS - 2))
                    pl.when(jnp.logical_not(inner))(functools.partial(wait_for, SPLITS - 1))
                else:
                    wait_for(SPLITS - 1)

        def gathered(head, kind):
            lane = (CHUNKS.index(chunk) * 3 + kind) * BLOCK
            lines = slice(head * part, (head + 1) * part)
            found = [pieces[image, source, lines, lane : lane + BLOCK] for source in range(SPLITS)]
            return jnp.concatenate(found, axis=0)

        with scope(f"attend_{image}{chunk}"):
            for head in range(small // part):
                query = (
                    column_norm(gathered(head, 0).astype(jnp.float32), q_gain[...])
                    * HEAD_DIM ** (-0.5)
                ).astype(jnp.bfloat16)
                key = column_norm(gathered(head, 1).astype(jnp.float32), k_gain[...]).astype(
                    jnp.bfloat16
                )
                scores = lax.dot_general(
                    key, query, (((0,), (0,)), ((), ())), preferred_element_type=jnp.float32
                )
                raised = jnp.exp(scores)
                weights = (raised / jnp.sum(raised, axis=0, keepdims=True)).astype(jnp.bfloat16)
                attended = jnp.dot(
                    gathered(head, 2), weights, preferred_element_type=jnp.float32
                ).astype(jnp.bfloat16)
                lane = context_lane + CHUNKS.index(chunk) * BLOCK
                for target in range(SPLITS):
                    line = image * PATCHES + target * small + head * part
                    work[line : line + part, lane : lane + BLOCK] = attended[
                        target * part : (target + 1) * part
                    ]
        for offset in (2, 1, 3):
            context_send(image, chunk, offset).start()
        returned[image, CHUNKS.index(chunk), quarter] = context_view(image, chunk, quarter)[...]

    def store(image, chunk):
        block = CHUNKS.index(chunk)
        with scope(f"w_context_{image}{chunk}"):
            view = returned.at[image, block, : SPLITS - 1]
            remote(
                view, view, context_out, context_got.at[image * 3 + block], quarter_at(1)
            ).wait_recv()
        out_ref[lines_of(image), block * BLOCK : (block + 1) * BLOCK] = (
            returned[image, block].reshape(BLOCK, PATCHES).T
        )

    def token_ready(image):
        with scope(f"w_token_{image}"):
            if image == 0:
                for piece in range(PIECES):
                    if piece < PIECES // 2:
                        relay(image, 1, piece).wait_recv()
                        relay(image, 2, piece).wait_recv()
                    else:
                        relay(image, 0, piece).wait_recv()
                        relay(image, 3, piece).wait_recv()
            else:
                relay(image, 1).wait_recv()
                relay(image, 2).wait_recv()

    def pass_quarter(image, piece=None):
        with scope(f"w_share_{image}"):
            share_send(image, piece).wait_recv()
        relay(image, 0, piece).start()

    def pass_group(image, piece=None):
        relay(image, 1, piece).start()

    def pass_near(image, piece=None):
        with scope(f"w_near_{image}"):
            relay(image, 0, piece).wait_recv()
        relay(image, 2, piece).start()

    def pass_side(image, piece):
        with scope(f"w_side_{image}"):
            relay(image, 1, piece).wait_recv()
        relay(image, 3, piece).start()

    def drain(view, semaphore):
        remote(view, view, semaphore, weight_got.at[0], sibling).wait_send()

    barrier = pltpu.get_barrier_semaphore()
    partners = [sibling, across, near_group] + [quarter_at(o) for o in range(1, SPLITS)]
    for device in partners:
        pl.semaphore_signal(barrier, inc=1, device_id=device, device_id_type=MESH)
    first_load().start()
    rest_load(1).start()
    rest_load(2).start()
    rest_load(3).start()
    for block in range(3):
        weight_load(block).start()
    for image in range(1, images):
        token_load(image).start()
    q_gain[...] = jnp.broadcast_to(q_gain_ref[...], (PATCHES, HEAD_DIM)).T
    k_gain[...] = jnp.broadcast_to(k_gain_ref[...], (PATCHES, HEAD_DIM)).T

    def share_norm(image, carry):
        normalize(image * PATCHES + quad_place * quad_rows, quad_rows, image * quad_rows)
        return carry

    first_load().wait()
    with scope("norm_share_0"):
        share_norm(0, 0)
    with scope("barrier"):
        pl.semaphore_wait(barrier, len(partners))
    for piece in range(PIECES):
        share_send(0, piece).start()
    weight_send(0).start()
    for block in range(3):
        weight_load(block).wait()
    with scope("fold"):
        swap_fold()

    @pl.when(inner)
    def _():
        for block in range(len(SWAPPED)):
            swap_send(block).start()

    rest_wait()
    token_load(1).wait()
    token_load(2).wait()
    with scope("norm_share"):
        lax.fori_loop(1, images, share_norm, 0)
    for image in range(1, images):
        share_send(image).start()
    weight_send(1).start()
    weight_send(2).start()

    def rest_norm(image, step, carry):
        normalize(image * PATCHES + (quad_place + step + 1) % 4 * quad_rows, quad_rows)
        return carry

    def rest_image(image, carry):
        with scope("norm_rest"):
            lax.fori_loop(0, 3, functools.partial(rest_norm, image), 0)

        @pl.when(image > 0)
        def _():
            pass_quarter(0, image - 1)
            pass_group(0, image - 1)

        return carry

    lax.fori_loop(0, images, rest_image, 0)
    pass_quarter(0, 2)
    pass_group(0, 2)
    pass_quarter(0, 3)
    pass_group(0, 3)
    pass_near(0, 0)
    pass_near(0, 1)
    swap_arrive(0)
    pass_side(0, 2)
    pass_side(0, 3)
    swap_finish(0)
    pass_quarter(1)
    pass_group(1)
    token_ready(0)
    send_partial(0, "a")
    own_chunk("a")
    sum_step(0, "a", 0)
    swap_arrive(1)
    swap_finish(1)
    send_partial(0, "b")
    pass_near(1)
    sum_step(0, "a", 1)
    sum_step(0, "a", 2)
    sum_keep(0, "a")
    pass_quarter(2)
    pass_group(2)
    own_chunk("b")
    swap_arrive(2)
    swap_finish(2)
    send_partial(0, "d")
    sum_up(0, "b")
    token_ready(1)
    send_partial(1, "a")
    send_partial(1, "b")
    send_partial(1, "d")
    own_chunk("d")
    attend(0, "a")
    pass_near(2)
    sum_up(0, "d")
    sum_up(1, "a")
    attend(0, "b")
    token_ready(2)
    send_partial(2, "a")
    send_partial(2, "b")
    send_partial(2, "d")
    sum_up(1, "b")
    attend(0, "d")
    sum_up(1, "d")
    attend(1, "a")
    sum_up(2, "a")
    attend(1, "b")
    sum_up(2, "b")
    attend(1, "d")
    sum_up(2, "d")
    attend(2, "a")
    for chunk in CHUNKS:
        store(0, chunk)
    store(1, "a")
    attend(2, "b")
    store(1, "b")
    attend(2, "d")
    store(1, "d")
    for chunk in CHUNKS:
        store(2, chunk)

    drain(weight.at[:, mine, :], weight_out)
    drain(share, share_out)
    drain(other.at[: images * 3 * quad_rows], relay_out)
    drain(work.at[:, :piece_lane], partial_out)
    drain(work.at[: images * small, :piece_lane], context_out)

    @pl.when(inner)
    def _():
        drain(got, swap_out)
        fewer = len(SWAPPED) * small
        drain(work.at[: images * 3 * small - images * fewer // 3, :piece_lane], piece_out)

    @pl.when(jnp.logical_not(inner))
    def _():
        drain(work.at[: images * 3 * small, :piece_lane], piece_out)


def fused(tokens, gain, weights, q_gain, k_gain):
    rows, features = tokens.shape
    kinds, depth, width = weights.shape
    images = rows // PATCHES
    small = BLOCK // SPLITS
    whole = pl.BlockSpec(memory_space=pltpu.VMEM)
    outside = pl.BlockSpec(memory_space=pl.ANY)
    dma = pltpu.SemaphoreType.DMA

    def vmem(*shape, dtype=jnp.bfloat16):
        return pltpu.VMEM(shape, dtype)

    share_count = PIECES + images - 1
    chunk_count = images * 3 + 2
    return pl.pallas_call(
        fused_kernel,
        out_shape=jax.ShapeDtypeStruct((rows, width), jnp.bfloat16),
        in_specs=[outside, whole, outside, whole, whole],
        out_specs=whole,
        scratch_shapes=[
            vmem(rows, features),
            vmem(kinds, 2 * depth, width),
            vmem(rows, features // 2),
            vmem(rows, features // 2),
            vmem(images * PATCHES // 4, features // 2),
            vmem(rows, kinds * width, dtype=jnp.float32),
            vmem(images, PATCHES, kinds * width),
            vmem(images, SPLITS, small, UNITS * PATCHES),
            vmem(images, 3, SPLITS, small, PATCHES),
            vmem(HEAD_DIM, PATCHES, dtype=jnp.float32),
            vmem(HEAD_DIM, PATCHES, dtype=jnp.float32),
            vmem(3 * len(SWAPPED), depth // 2, 2 * small),
            vmem(2, 3 * len(SWAPPED), depth // 2, 2 * small),
            dma((images + 1,)), dma((3,)), dma, dma((3,)),
            dma, dma((6,)),
            dma, dma((share_count,)),
            dma, dma((4 * share_count,)),
            dma, dma((chunk_count,)),
            dma, dma((chunk_count,)),
            dma, dma((images * 3,)),
        ],
        compiler_params=pltpu.CompilerParams(
            collective_id=0, has_side_effects=True, vmem_limit_bytes=VMEM_LIMIT
        ),
        name="fused",
    )(tokens, gain.reshape(1, features), weights, q_gain.reshape(1, HEAD_DIM),
      k_gain.reshape(1, HEAD_DIM))


def body(tokens, ln_gain, w_qkv, q_gain, k_gain):
    fits = lax.axis_size("dp") == 4 and lax.axis_size("mp") == GROUPS * SPLITS
    fits = fits and tokens.shape == (3 * PATCHES, 4 * w_qkv.shape[0])
    fits = fits and w_qkv.shape[1:] == (3, 3 * BLOCK) and w_qkv.shape[0] % BLOCK == 0
    if not fits:
        return plain_body(tokens, ln_gain, w_qkv, q_gain, k_gain)
    return fused(tokens, ln_gain, jnp.transpose(w_qkv, (1, 0, 2)), q_gain, k_gain)


def solution(mesh):
    return jax.shard_map(
        body,
        mesh=mesh,
        in_specs=(P("dp", None), P(), P("dp", None, "mp"), P(), P()),
        out_specs=P("dp", "mp"),
        check_vma=False,
    )
```

```python
import functools

import jax
import jax.numpy as jnp
from jax import lax
from jax.experimental import pallas as pl
from jax.experimental.pallas import tpu as pltpu
from jax.sharding import PartitionSpec as P


HEADS = 48
HEAD_DIM = 128
PATCHES = 256
SPLITS = 4


norm_eps = 1e-06


def from_behind(shard, axis, by):
    length = lax.axis_size(axis)
    return lax.ppermute(shard, axis, [(i, (i + by) % length) for i in range(length)])


def layer_norm(values, gain_vector):
    centre = jnp.mean(values, axis=-1, keepdims=True)
    centred = values - centre
    spread = jnp.mean(centred * centred, axis=-1, keepdims=True)
    return centred * lax.rsqrt(spread + norm_eps) * gain_vector


def head_norm(pieces, gain_rows):
    values = pieces.astype(jnp.float32)
    centre = jnp.mean(values, axis=(0, 4), keepdims=True)
    centred = values - centre
    spread = jnp.mean(centred * centred, axis=(0, 4), keepdims=True)
    return centred * lax.rsqrt(spread + norm_eps) * gain_rows[:, None, None, None, :]


def ordered_gains(gain_vector, quarter_order):
    gain_table = gain_vector.reshape(SPLITS, -1)
    selector = (quarter_order[:, None] == jnp.arange(SPLITS, dtype=jnp.int32)[None, :]).astype(
        jnp.float32
    )
    return jnp.dot(selector, gain_table, precision=lax.Precision.HIGHEST)


def plain_body(tokens, ln_gain, w_qkv, q_gain, k_gain):
    local_rows = tokens.shape[0]
    normed = layer_norm(tokens.astype(jnp.float32), ln_gain).astype(jnp.bfloat16)
    flat_weight = w_qkv.reshape(w_qkv.shape[0], -1)
    out_width = flat_weight.shape[1]
    row_piece = lax.all_gather(w_qkv, "dp", axis=0, tiled=True)
    partial_value = jnp.dot(
        normed, row_piece.reshape(row_piece.shape[0], out_width), preferred_element_type=jnp.float32
    )
    projected = partial_value.astype(jnp.bfloat16)
    groups = lax.axis_size("mp") // SPLITS
    head_count = HEADS // groups
    quarter_rows = PATCHES // SPLITS
    my_quarter = lax.axis_index("mp") // groups
    images = local_rows // PATCHES
    head_view = projected.reshape(images, PATCHES, 3, head_count, HEAD_DIM // SPLITS)
    queries = head_view[:, :, 0]
    keys_vals = head_view[:, :, 1:]
    counting = jnp.arange(SPLITS, dtype=jnp.int32)
    own_rows = lax.dynamic_slice_in_dim(queries, my_quarter * quarter_rows, quarter_rows, 1)
    query_list = [own_rows]
    pair_list = [keys_vals]
    for offset in range(1, SPLITS):
        outgoing = lax.dynamic_slice_in_dim(
            queries, (my_quarter + offset) % SPLITS * quarter_rows, quarter_rows, 1
        )
        got_query, got_pair = from_behind((outgoing, keys_vals), "mp", offset * groups)
        query_list.append(got_query)
        pair_list.append(got_pair)
    query_pieces = jnp.stack(query_list, 0)
    pair_pieces = jnp.stack(pair_list, 0)
    quarter_order = (my_quarter - counting) % SPLITS
    query_normed = (
        head_norm(query_pieces, ordered_gains(q_gain, quarter_order)) * HEAD_DIM ** (-0.5)
    ).astype(jnp.bfloat16)
    key_normed = head_norm(pair_pieces[:, :, :, 0], ordered_gains(k_gain, quarter_order)).astype(
        jnp.bfloat16
    )
    value_part = pair_pieces[:, :, :, 1]
    scores = jnp.einsum(
        "sirhe,sikhe->ihrk", query_normed, key_normed, preferred_element_type=jnp.float32
    )
    raised = jnp.exp(scores)
    weights = (raised / jnp.sum(raised, axis=-1, keepdims=True)).astype(jnp.bfloat16)
    context = jnp.einsum(
        "ihrk,sikhe->sirhe", weights, value_part, preferred_element_type=jnp.float32
    ).astype(jnp.bfloat16)
    rows_list = [context[0]]
    for offset in range(1, SPLITS):
        wanted = (my_quarter - offset) % SPLITS
        slot_index = jnp.sum(jnp.where(quarter_order == wanted, counting, 0))
        outgoing = lax.dynamic_index_in_dim(context, slot_index, 0, keepdims=False)
        rows_list.append(from_behind(outgoing, "mp", (SPLITS - offset) * groups))
    own_block = jnp.roll(jnp.concatenate(rows_list, 1), my_quarter * quarter_rows, axis=1)
    return own_block.reshape(local_rows, -1)

MESH = pl.DeviceIdType.MESH
VMEM_LIMIT = 62 * 1024 * 1024
BLOCK = 256
PIECES = 4
GROUPS = 2
UNITS = 9
CHUNKS = "abd"
SWAPPED = "abd"


def column_norm(values, gain):
    centre = jnp.mean(values, axis=0, keepdims=True)
    centred = values - centre
    spread = jnp.mean(centred * centred, axis=0, keepdims=True)
    return centred * lax.rsqrt(spread + norm_eps) * gain


def span(start, size):
    return pl.ds(pl.multiple_of(start, size), size)


def fused_kernel(
    token_hbm, gain_ref, weight_hbm, q_gain_ref, k_gain_ref, out_ref,
    work, weight, own, other, share, total, partial, pieces, returned,
    q_gain, k_gain, swap, got,
    token_in, weight_in, weight_out, weight_got, swap_out, swap_got,
    share_out, share_got, relay_out, relay_got, partial_out, partial_got,
    piece_out, piece_got, context_out, context_got,
):
    scope = jax.named_scope
    dp, mp = lax.axis_index("dp"), lax.axis_index("mp")
    side, core = dp // 2, dp % 2
    quarter, group = mp // GROUPS, mp % GROUPS
    rows, features = token_hbm.shape
    depth, width = weight_hbm.shape[1:]
    half = features // 2
    images = rows // PATCHES
    part = HEAD_DIM // SPLITS
    quad_rows = PATCHES // 4
    piece_rows = quad_rows // PIECES
    small = BLOCK // SPLITS
    folded = depth // 2
    piece_lane = UNITS * BLOCK
    context_lane = 2 * piece_lane

    sibling = (side * 2 + 1 - core, mp)
    across = ((1 - side) * 2 + core, mp)
    near_group = (dp, quarter * GROUPS + 1 - group)
    near_quarter = (dp, (quarter + 1 - 2 * (quarter % 2)) * GROUPS + group)
    quad_place = (quarter % 2) * 2 + group
    near_place = (1 - quarter % 2) * 2 + group

    def quarter_at(offset):
        return (dp, (quarter + offset) % SPLITS * GROUPS + group)

    def remote(source, target, send, receive, device):
        return pltpu.make_async_remote_copy(
            src_ref=source, dst_ref=target, send_sem=send, recv_sem=receive,
            device_id=device, device_id_type=MESH,
        )

    def lines_of(image):
        return slice(image * PATCHES, (image + 1) * PATCHES)

    def token_load(image):
        lines = lines_of(image)
        return pltpu.make_async_copy(token_hbm.at[lines], work.at[lines], token_in.at[image])

    def quarter_load(turn, semaphore):
        lines = span((quad_place + turn) % 4 * quad_rows, quad_rows)
        return pltpu.make_async_copy(token_hbm.at[lines], work.at[lines], semaphore)

    def first_load():
        return quarter_load(0, token_in.at[0])

    def rest_load(turn):
        return quarter_load(turn, token_in.at[3])

    def rest_wait():
        lines = slice(0, 3 * quad_rows)
        pltpu.make_async_copy(token_hbm.at[lines], work.at[lines], token_in.at[3]).wait()

    mine = span(core * depth, depth)

    def block_lanes(block):
        return slice(block * BLOCK, (block + 1) * BLOCK)

    def weight_load(block):
        columns = block_lanes(block)
        return pltpu.make_async_copy(
            weight_hbm.at[:, :, columns], weight.at[:, mine, columns], weight_in.at[block]
        )

    def weight_send(block):
        columns = block_lanes(block)
        return remote(
            weight_hbm.at[:, :, columns], weight.at[:, mine, columns],
            weight_out, weight_got.at[block], sibling,
        )

    inner = (quarter == 1) | (quarter == 2)
    partner = 3 - quarter

    def units_of(block):
        return slice(block * 3, block * 3 + 3)

    def swap_send(block):
        view = units_of(block)
        return remote(
            swap.at[view], got.at[0, view], swap_out, swap_got.at[block],
            (dp, partner * GROUPS + group),
        )

    def swap_pass(block):
        view = units_of(block)
        return remote(
            got.at[0, view], got.at[1, view],
            swap_out, swap_got.at[3 + block], sibling,
        )

    def swap_lanes(block, here):
        first = block * BLOCK + (2 * small if here == 1 else 0)
        return slice(first, first + 2 * small)

    def swap_fold():
        for here, side in ((1, 0), (2, 1)):
            @pl.when(quarter == here)
            def _(here=here, side=side):
                for unit in range(3 * len(SWAPPED)):
                    block, kind = divmod(unit, 3)
                    lanes = swap_lanes(block, here)
                    swap[unit] = jnp.concatenate(
                        [
                            weight[kind, span(core * depth + row * folded, folded), lanes][
                                :, side * small : (side + 1) * small
                            ]
                            for row in range(2)
                        ],
                        axis=1,
                    )

    def swap_unfold(block, slot):
        owner = core if slot == 0 else 1 - core
        for here, side in ((1, 0), (2, 1)):
            @pl.when(quarter == here)
            def _(here=here, side=side):
                for kind in range(3):
                    lanes = swap_lanes(block, here)
                    for row in range(2):
                        lines = span(owner * depth + row * folded, folded)
                        fresh = got[slot, block * 3 + kind][:, row * small : (row + 1) * small]
                        held = weight[kind, lines, lanes][
                            :, (1 - side) * small : (2 - side) * small
                        ]
                        both = (fresh, held) if side == 0 else (held, fresh)
                        weight[kind, lines, lanes] = jnp.concatenate(both, axis=1)

    def swap_arrive(block):
        if block >= len(SWAPPED):
            weight_send(block).wait_recv()
            return
        with scope("w_swap"):
            weight_send(block).wait_recv()

            @pl.when(inner)
            def _():
                swap_send(block).wait_recv()
                swap_pass(block).start()

    def swap_finish(block):
        if block >= len(SWAPPED):
            return
        with scope("swap_finish"):
            @pl.when(inner)
            def _():
                swap_unfold(block, 0)
                swap_pass(block).wait_recv()
                swap_unfold(block, 1)

    def unless_swapped(chunk, offset, action):
        if offset == 2 or chunk not in SWAPPED:
            action()
        else:
            pl.when(quarter != (1 if offset == 1 else 2))(action)

    def quad_view(image, place, piece=None):
        line = image * PATCHES + place * quad_rows
        if piece is None:
            return other.at[span(line, quad_rows)]
        return other.at[span(line + piece * piece_rows, piece_rows)]

    def share_slot(image, piece):
        return piece if piece is not None else PIECES + image - 1

    def share_send(image, piece=None):
        if piece is None:
            source = share.at[image * quad_rows : (image + 1) * quad_rows]
        else:
            source = share.at[span(image * quad_rows + piece * piece_rows, piece_rows)]
        slot = share_slot(image, piece)
        return remote(
            source, quad_view(image, quad_place, piece),
            share_out, share_got.at[slot], across,
        )

    def relay(image, way, piece=None):
        places = (quad_place, quad_place, near_place, quad_place + 1 - 2 * group)
        view = quad_view(image, places[way], piece)
        slot = share_slot(image, piece) * 4 + way
        device = near_group if way in (1, 2) else near_quarter
        return remote(view, view, relay_out, relay_got.at[slot], device)

    def parts_of(image, chunk):
        first = CHUNKS.index(chunk) * 3
        if (image, chunk) in ((0, "a"), (images - 1, CHUNKS[-1])):
            return [(unit, 1) for unit in range(first, first + 3)]
        return [(first, 3)]

    def chunk_slot(image, chunk, step):
        slot = step
        for earlier in range(images):
            for other_chunk in CHUNKS:
                if (earlier, other_chunk) == (image, chunk):
                    return slot
                slot += len(parts_of(earlier, other_chunk))

    def partial_send(image, chunk, step):
        first, count = parts_of(image, chunk)[step]
        columns = slice(first * BLOCK, (first + count) * BLOCK)
        slot = chunk_slot(image, chunk, step)
        return remote(
            work.at[lines_of(image), columns], partial.at[image, :, columns],
            partial_out, partial_got.at[slot], across,
        )

    def piece_view(image, target, first, count):
        lane = piece_lane + first * BLOCK
        return work.at[
            span(image * PATCHES + target * small, small), slice(lane, lane + count * BLOCK)
        ]

    def piece_send(image, chunk, step, offset):
        first, count = parts_of(image, chunk)[step]
        slot = chunk_slot(image, chunk, step)
        return remote(
            piece_view(image, (quarter + offset) % SPLITS, first, count),
            pieces.at[image, quarter, :, first * BLOCK : (first + count) * BLOCK],
            piece_out, piece_got.at[slot], quarter_at(offset),
        )

    def context_view(image, chunk, target):
        lane = context_lane + CHUNKS.index(chunk) * BLOCK
        return work.at[span(image * PATCHES + target * small, small), slice(lane, lane + BLOCK)]

    def context_send(image, chunk, offset):
        slot = image * 3 + CHUNKS.index(chunk)
        return remote(
            context_view(image, chunk, (quarter + offset) % SPLITS),
            returned.at[image, CHUNKS.index(chunk), quarter],
            context_out, context_got.at[slot], quarter_at(offset),
        )

    own_half = span(side * half, half)
    other_half = span((1 - side) * half, half)

    def normalize(line, count, share_line=None):
        lines = span(line, count)
        values = work[lines, :].astype(jnp.float32)
        centre = jnp.mean(values, axis=-1, keepdims=True)
        centred = values - centre
        spread = jnp.mean(centred * centred, axis=-1, keepdims=True)
        scale = lax.rsqrt(spread + norm_eps)

        def scaled(columns):
            return (
                (work[lines, columns].astype(jnp.float32) - centre) * scale * gain_ref[:, columns]
            ).astype(jnp.bfloat16)

        if share_line is not None:
            share[span(share_line, count), :] = scaled(other_half)
        own[lines, :] = scaled(own_half)

    def own_part(block, step):
        with scope("own_part"):
            total[:, span((block * 3 + step) * BLOCK, BLOCK)] = jnp.dot(
                own[...], weight[step, :, block_lanes(block)], preferred_element_type=jnp.float32
            )

    def own_chunk(chunk):
        def looped(step, carry):
            own_part(CHUNKS.index(chunk), step)
            return carry

        lax.fori_loop(0, 3, looped, 0)

    def send_partial(image, chunk):
        block = CHUNKS.index(chunk)
        split = len(parts_of(image, chunk)) > 1

        def other_part(step):
            work[lines_of(image), span((block * 3 + step) * BLOCK, BLOCK)] = jnp.dot(
                other[lines_of(image), :], weight[step, :, block_lanes(block)],
                preferred_element_type=jnp.float32,
            ).astype(jnp.bfloat16)

        def looped(step, carry):
            other_part(step)
            return carry

        with scope(f"other_part_{image}{chunk}"):
            if split:
                for step in range(3):
                    other_part(step)
                    partial_send(image, chunk, step).start()
            else:
                lax.fori_loop(0, 3, looped, 0)
                partial_send(image, chunk, 0).start()

    def sum_step(image, chunk, step):
        first, count = parts_of(image, chunk)[step]
        with scope(f"w_partial_{image}{chunk}"):
            partial_send(image, chunk, step).wait_recv()
        for unit in range(first, first + count):
            columns = slice(unit * BLOCK, (unit + 1) * BLOCK)
            whole = total[lines_of(image), columns] + partial[image, :, columns].astype(
                jnp.float32
            )
            work[
                lines_of(image), piece_lane + unit * BLOCK : piece_lane + (unit + 1) * BLOCK
            ] = whole.T.astype(jnp.bfloat16)
        for offset in (2, 1, 3):
            unless_swapped(
                chunk, offset, lambda offset=offset: piece_send(image, chunk, step, offset).start()
            )

    def sum_up(image, chunk):
        for step in range(len(parts_of(image, chunk))):
            sum_step(image, chunk, step)
        sum_keep(image, chunk)

    def sum_keep(image, chunk):
        first = CHUNKS.index(chunk) * 3
        lanes = slice(first * BLOCK, (first + 3) * BLOCK)
        pieces[image, quarter, :, lanes] = piece_view(image, quarter, first, 3)[...]

        if chunk in SWAPPED:
            @pl.when(inner)
            def _():
                pieces[image, partner, :, lanes] = piece_view(image, partner, first, 3)[...]

    def attend(image, chunk):
        with scope(f"w_piece_{image}{chunk}"):
            for step, (first, count) in enumerate(parts_of(image, chunk)):
                slot = chunk_slot(image, chunk, step)
                lanes = slice(first * BLOCK, (first + count) * BLOCK)

                def wait_for(number, slot=slot, lanes=lanes):
                    view = pieces.at[image, :number, :, lanes]
                    remote(view, view, piece_out, piece_got.at[slot], quarter_at(1)).wait_recv()

                if chunk in SWAPPED:
                    pl.when(inner)(functools.partial(wait_for, SPLITS - 2))
                    pl.when(jnp.logical_not(inner))(functools.partial(wait_for, SPLITS - 1))
                else:
                    wait_for(SPLITS - 1)

        def gathered(head, kind):
            lane = (CHUNKS.index(chunk) * 3 + kind) * BLOCK
            lines = slice(head * part, (head + 1) * part)
            found = [pieces[image, source, lines, lane : lane + BLOCK] for source in range(SPLITS)]
            return jnp.concatenate(found, axis=0)

        with scope(f"attend_{image}{chunk}"):
            for head in range(small // part):
                query = (
                    column_norm(gathered(head, 0).astype(jnp.float32), q_gain[...])
                    * HEAD_DIM ** (-0.5)
                ).astype(jnp.bfloat16)
                key = column_norm(gathered(head, 1).astype(jnp.float32), k_gain[...]).astype(
                    jnp.bfloat16
                )
                scores = lax.dot_general(
                    key, query, (((0,), (0,)), ((), ())), preferred_element_type=jnp.float32
                )
                raised = jnp.exp(scores)
                weights = (raised / jnp.sum(raised, axis=0, keepdims=True)).astype(jnp.bfloat16)
                attended = jnp.dot(
                    gathered(head, 2), weights, preferred_element_type=jnp.float32
                ).astype(jnp.bfloat16)
                lane = context_lane + CHUNKS.index(chunk) * BLOCK
                for target in range(SPLITS):
                    line = image * PATCHES + target * small + head * part
                    work[line : line + part, lane : lane + BLOCK] = attended[
                        target * part : (target + 1) * part
                    ]
        for offset in (2, 1, 3):
            context_send(image, chunk, offset).start()
        returned[image, CHUNKS.index(chunk), quarter] = context_view(image, chunk, quarter)[...]

    def store(image, chunk):
        block = CHUNKS.index(chunk)
        with scope(f"w_context_{image}{chunk}"):
            view = returned.at[image, block, : SPLITS - 1]
            remote(
                view, view, context_out, context_got.at[image * 3 + block], quarter_at(1)
            ).wait_recv()
        out_ref[lines_of(image), block * BLOCK : (block + 1) * BLOCK] = (
            returned[image, block].reshape(BLOCK, PATCHES).T
        )

    def token_ready(image):
        with scope(f"w_token_{image}"):
            if image == 0:
                for piece in range(PIECES):
                    if piece < PIECES // 2:
                        relay(image, 1, piece).wait_recv()
                        relay(image, 2, piece).wait_recv()
                    else:
                        relay(image, 0, piece).wait_recv()
                        relay(image, 3, piece).wait_recv()
            else:
                relay(image, 1).wait_recv()
                relay(image, 2).wait_recv()

    def pass_quarter(image, piece=None):
        with scope(f"w_share_{image}"):
            share_send(image, piece).wait_recv()
        relay(image, 0, piece).start()

    def pass_group(image, piece=None):
        relay(image, 1, piece).start()

    def pass_near(image, piece=None):
        with scope(f"w_near_{image}"):
            relay(image, 0, piece).wait_recv()
        relay(image, 2, piece).start()

    def pass_side(image, piece):
        with scope(f"w_side_{image}"):
            relay(image, 1, piece).wait_recv()
        relay(image, 3, piece).start()

    def drain(view, semaphore):
        remote(view, view, semaphore, weight_got.at[0], sibling).wait_send()

    barrier = pltpu.get_barrier_semaphore()
    partners = [sibling, across, near_group] + [quarter_at(o) for o in range(1, SPLITS)]
    for device in partners:
        pl.semaphore_signal(barrier, inc=1, device_id=device, device_id_type=MESH)
    first_load().start()
    rest_load(1).start()
    rest_load(2).start()
    rest_load(3).start()
    for block in range(3):
        weight_load(block).start()
    for image in range(1, images):
        token_load(image).start()
    q_gain[...] = jnp.broadcast_to(q_gain_ref[...], (PATCHES, HEAD_DIM)).T
    k_gain[...] = jnp.broadcast_to(k_gain_ref[...], (PATCHES, HEAD_DIM)).T

    def share_norm(image, carry):
        normalize(image * PATCHES + quad_place * quad_rows, quad_rows, image * quad_rows)
        return carry

    first_load().wait()
    with scope("norm_share_0"):
        share_norm(0, 0)
    with scope("barrier"):
        pl.semaphore_wait(barrier, len(partners))
    for piece in range(PIECES):
        share_send(0, piece).start()
    weight_send(0).start()
    for block in range(3):
        weight_load(block).wait()
    with scope("fold"):
        swap_fold()

    @pl.when(inner)
    def _():
        for block in range(len(SWAPPED)):
            swap_send(block).start()

    rest_wait()
    token_load(1).wait()
    token_load(2).wait()
    with scope("norm_share"):
        lax.fori_loop(1, images, share_norm, 0)
    for image in range(1, images):
        share_send(image).start()
    weight_send(1).start()
    weight_send(2).start()

    def rest_norm(image, step, carry):
        normalize(image * PATCHES + (quad_place + step + 1) % 4 * quad_rows, quad_rows)
        return carry

    def rest_image(image, carry):
        with scope("norm_rest"):
            lax.fori_loop(0, 3, functools.partial(rest_norm, image), 0)

        @pl.when(image > 0)
        def _():
            pass_quarter(0, image - 1)
            pass_group(0, image - 1)

        return carry

    lax.fori_loop(0, images, rest_image, 0)
    pass_quarter(0, 2)
    pass_group(0, 2)
    pass_quarter(0, 3)
    pass_group(0, 3)
    pass_near(0, 0)
    pass_near(0, 1)
    swap_arrive(0)
    pass_side(0, 2)
    pass_side(0, 3)
    swap_finish(0)
    pass_quarter(1)
    pass_group(1)
    token_ready(0)
    send_partial(0, "a")
    own_chunk("a")
    sum_step(0, "a", 0)
    swap_arrive(1)
    swap_finish(1)
    send_partial(0, "b")
    pass_near(1)
    sum_step(0, "a", 1)
    sum_step(0, "a", 2)
    sum_keep(0, "a")
    pass_quarter(2)
    pass_group(2)
    own_chunk("b")
    swap_arrive(2)
    swap_finish(2)
    send_partial(0, "d")
    sum_up(0, "b")
    token_ready(1)
    send_partial(1, "a")
    send_partial(1, "b")
    send_partial(1, "d")
    own_chunk("d")
    attend(0, "a")
    pass_near(2)
    sum_up(0, "d")
    sum_up(1, "a")
    attend(0, "b")
    token_ready(2)
    send_partial(2, "a")
    send_partial(2, "b")
    send_partial(2, "d")
    sum_up(1, "b")
    attend(0, "d")
    sum_up(1, "d")
    attend(1, "a")
    sum_up(2, "a")
    attend(1, "b")
    sum_up(2, "b")
    attend(1, "d")
    sum_up(2, "d")
    attend(2, "a")
    for chunk in CHUNKS:
        store(0, chunk)
    store(1, "a")
    attend(2, "b")
    store(1, "b")
    attend(2, "d")
    store(1, "d")
    for chunk in CHUNKS:
        store(2, chunk)

    drain(weight.at[:, mine, :], weight_out)
    drain(share, share_out)
    drain(other.at[: images * 3 * quad_rows], relay_out)
    drain(work.at[:, :piece_lane], partial_out)
    drain(work.at[: images * small, :piece_lane], context_out)

    @pl.when(inner)
    def _():
        drain(got, swap_out)
        fewer = len(SWAPPED) * small
        drain(work.at[: images * 3 * small - images * fewer // 3, :piece_lane], piece_out)

    @pl.when(jnp.logical_not(inner))
    def _():
        drain(work.at[: images * 3 * small, :piece_lane], piece_out)


def fused(tokens, gain, weights, q_gain, k_gain):
    rows, features = tokens.shape
    kinds, depth, width = weights.shape
    images = rows // PATCHES
    small = BLOCK // SPLITS
    whole = pl.BlockSpec(memory_space=pltpu.VMEM)
    outside = pl.BlockSpec(memory_space=pl.ANY)
    dma = pltpu.SemaphoreType.DMA

    def vmem(*shape, dtype=jnp.bfloat16):
        return pltpu.VMEM(shape, dtype)

    share_count = PIECES + images - 1
    chunk_count = images * 3 + 4
    return pl.pallas_call(
        fused_kernel,
        out_shape=jax.ShapeDtypeStruct((rows, width), jnp.bfloat16),
        in_specs=[outside, whole, outside, whole, whole],
        out_specs=whole,
        scratch_shapes=[
            vmem(rows, features),
            vmem(kinds, 2 * depth, width),
            vmem(rows, features // 2),
            vmem(rows, features // 2),
            vmem(images * PATCHES // 4, features // 2),
            vmem(rows, kinds * width, dtype=jnp.float32),
            vmem(images, PATCHES, kinds * width),
            vmem(images, SPLITS, small, UNITS * PATCHES),
            vmem(images, 3, SPLITS, small, PATCHES),
            vmem(HEAD_DIM, PATCHES, dtype=jnp.float32),
            vmem(HEAD_DIM, PATCHES, dtype=jnp.float32),
            vmem(3 * len(SWAPPED), depth // 2, 2 * small),
            vmem(2, 3 * len(SWAPPED), depth // 2, 2 * small),
            dma((images + 1,)), dma((3,)), dma, dma((3,)),
            dma, dma((6,)),
            dma, dma((share_count,)),
            dma, dma((4 * share_count,)),
            dma, dma((chunk_count,)),
            dma, dma((chunk_count,)),
            dma, dma((images * 3,)),
        ],
        compiler_params=pltpu.CompilerParams(
            collective_id=0, has_side_effects=True, vmem_limit_bytes=VMEM_LIMIT
        ),
        name="fused",
    )(tokens, gain.reshape(1, features), weights, q_gain.reshape(1, HEAD_DIM),
      k_gain.reshape(1, HEAD_DIM))


def body(tokens, ln_gain, w_qkv, q_gain, k_gain):
    fits = lax.axis_size("dp") == 4 and lax.axis_size("mp") == GROUPS * SPLITS
    fits = fits and tokens.shape == (3 * PATCHES, 4 * w_qkv.shape[0])
    fits = fits and w_qkv.shape[1:] == (3, 3 * BLOCK) and w_qkv.shape[0] % BLOCK == 0
    if not fits:
        return plain_body(tokens, ln_gain, w_qkv, q_gain, k_gain)
    return fused(tokens, ln_gain, jnp.transpose(w_qkv, (1, 0, 2)), q_gain, k_gain)


def solution(mesh):
    return jax.shard_map(
        body,
        mesh=mesh,
        in_specs=(P("dp", None), P(), P("dp", None, "mp"), P(), P()),
        out_specs=P("dp", "mp"),
        check_vma=False,
    )
```
